32 devices in a mesh: cond: 2 (over core), kern: 2 (over y), tile: 8 (over z, x).
Axes of the slice: x: 2, y: 2, z: 4, core: 2. Of those that a mesh axis runs over, the one named last changes fastest.
Arguments:
- mask: bfloat16 [1, 1024, 1024], P(None, 'tile'), may hold values from -6 to 6
- kernels: bfloat16 [2, 4, 24, 512, 512], P(None, 'cond', 'kern', 'tile'), may hold values from -6 to 6
- kernel_weights: float32 [4, 24], P('cond', 'kern'), may hold values from 0.02 to 0.2
Outputs:
- low: float32 [1, 1024, 1024], P(None, 'tile', 'kern')
- high: float32 [1, 1024, 1024], P(None, 'tile', 'kern')
The draws below stay inside these ranges and needn't reach their ends.
All inputs are finite; a program needn't handle non-finite values.
Results may differ from the reference program's by a relative error of at most 0.0032.
Values may be sent and summed in bfloat16 or wider, within the bound.
A program may use at most 128 MiB of HBM per device.

```python
import math
import jax
import jax.numpy as jnp
from jax import lax

P_SIZE = 1024
B = 512
KERNELS = 24
CONDS = 4
TILES = 1


def steps_of(own_key, shape, split, smallest, largest):
    factor_of = 1.0
    for dim, parts in split:
        steps = jax.random.uniform(jax.random.fold_in(jax.random.fold_in(own_key, 6), dim), (parts,), jnp.float32, smallest / len(split), largest / len(split))
        factor_of = factor_of * jnp.repeat(jnp.exp(steps), shape[dim] // parts).reshape((-1,) + (1,) * (len(shape) - 1 - dim))
    return factor_of


def normal_values(own_key, dims, scale, most, split=(), held_as=jnp.bfloat16):
    values = scale * jax.random.normal(own_key, dims, jnp.float32)
    if split:
        values = values * steps_of(own_key, dims, split, -0.22, 0.18)
    return jnp.clip(values, -most, most).astype(held_as)


def setup_inputs(seed: int = 0) -> dict:
    keys = jax.random.split(jax.random.key(seed), 4)
    return {
        "mask": normal_values(keys[0], (TILES, P_SIZE, P_SIZE), 1.0, 6.0, ((1, 8),)),
        "kernels": normal_values(keys[1], (2, CONDS, KERNELS, B, B), 1.0, 6.0, ((1, 2), (2, 2), (3, 8))),
        "kernel_weights": jnp.clip(jnp.exp(math.log(0.2) - 2.3025851 * jax.random.uniform(keys[2], (CONDS, KERNELS), jnp.float32) ** steps_of(keys[2], (CONDS, KERNELS), ((0, 2), (1, 2)), -0.2, 0.2)), 0.02, 0.2),
    }


def tables(length, count):
    pixel = jnp.arange(length, dtype=jnp.int32)[:, None]
    freq = jnp.arange(count, dtype=jnp.int32)[None, :] - count // 2
    phase = jnp.mod(pixel * freq, length).astype(jnp.float32) * (2.0 * math.pi / length)
    factor = 1.0 / math.sqrt(length)
    return ((jnp.cos(phase) * factor).astype(jnp.bfloat16), (jnp.sin(phase) * factor).astype(jnp.bfloat16))

def product(left, right):
    return jnp.dot(left, right, preferred_element_type=jnp.float32)

def reference(mask, kernels, kernel_weights):
    cos_table, sin_table = tables(P_SIZE, B)
    cos_back = cos_table.T
    sin_back = sin_table.T

    def one_tile(tile):
        row_re = product(tile, cos_table).astype(jnp.bfloat16)
        row_im = (-product(tile, sin_table)).astype(jnp.bfloat16)
        spec_re = product(row_re.T, cos_table) + product(row_im.T, sin_table)
        spec_im = product(row_im.T, cos_table) - product(row_re.T, sin_table)

        def one_cond(inputs):
            cond_re, cond_im, weights = inputs

            def add_kernel(total, item):
                kern_re, kern_im, weight = item
                kern_re = kern_re.astype(jnp.float32)
                kern_im = kern_im.astype(jnp.float32)
                filt_re = (spec_re * kern_re - spec_im * kern_im).astype(jnp.bfloat16)
                filt_im = (spec_re * kern_im + spec_im * kern_re).astype(jnp.bfloat16)
                half_re = (product(filt_re, cos_back) - product(filt_im, sin_back)).astype(jnp.bfloat16)
                half_im = (product(filt_re, sin_back) + product(filt_im, cos_back)).astype(jnp.bfloat16)
                field_re = product(half_re.T, cos_back) - product(half_im.T, sin_back)
                field_im = product(half_re.T, sin_back) + product(half_im.T, cos_back)
                return (total + weight * (field_re * field_re + field_im * field_im), None)
            start = jnp.zeros((P_SIZE, P_SIZE), jnp.float32)
            total, _ = lax.scan(add_kernel, start, (cond_re, cond_im, weights))
            return total
        intensity = lax.map(one_cond, (kernels[0], kernels[1], kernel_weights))
        return (lax.optimization_barrier(jnp.min(intensity, axis=0)), lax.optimization_barrier(jnp.max(intensity, axis=0)))
    low, high = lax.map(one_tile, mask)
    return (low, high)
```

```python
import functools
import math

import jax
import jax.numpy as jnp
import numpy as np
from jax import lax
from jax.experimental import pallas as pl
from jax.experimental.pallas import tpu as pltpu
from jax.sharding import PartitionSpec as P


def tables(length, count):
    pixel = jnp.arange(length, dtype=jnp.int32)[:, None]
    freq = jnp.arange(count, dtype=jnp.int32)[None, :] - count // 2
    phase = jnp.mod(pixel * freq, length).astype(jnp.float32) * (2.0 * math.pi / length)
    factor = 1.0 / math.sqrt(length)
    return (
        (jnp.cos(phase) * factor).astype(jnp.bfloat16),
        (jnp.sin(phase) * factor).astype(jnp.bfloat16),
    )


def field_power(half_re, half_im, cos_table, sin_table):
    field_re = jnp.einsum("tnjr,pj->tnrp", half_re, cos_table, preferred_element_type=jnp.float32)
    field_re = field_re - jnp.einsum(
        "tnjr,pj->tnrp", half_im, sin_table, preferred_element_type=jnp.float32
    )
    field_im = jnp.einsum("tnjr,pj->tnrp", half_re, sin_table, preferred_element_type=jnp.float32)
    field_im = field_im + jnp.einsum(
        "tnjr,pj->tnrp", half_im, cos_table, preferred_element_type=jnp.float32
    )
    return field_re * field_re + field_im * field_im


def filter_spectrum(spec_re, spec_im, kern_re, kern_im):
    kern_re = kern_re.astype(jnp.float32)
    kern_im = kern_im.astype(jnp.float32)
    filt_re = spec_re[:, None] * kern_re[None] - spec_im[:, None] * kern_im[None]
    filt_im = spec_re[:, None] * kern_im[None] + spec_im[:, None] * kern_re[None]
    return (filt_re.astype(jnp.bfloat16), filt_im.astype(jnp.bfloat16))


def half_transform(filt_re, filt_im, cos_part, sin_part):
    half_re = jnp.einsum("tnji,ri->tnjr", filt_re, cos_part, preferred_element_type=jnp.float32)
    half_re = half_re - jnp.einsum(
        "tnji,ri->tnjr", filt_im, sin_part, preferred_element_type=jnp.float32
    )
    half_im = jnp.einsum("tnji,ri->tnjr", filt_re, sin_part, preferred_element_type=jnp.float32)
    half_im = half_im + jnp.einsum(
        "tnji,ri->tnjr", filt_im, cos_part, preferred_element_type=jnp.float32
    )
    return (half_re.astype(jnp.bfloat16), half_im.astype(jnp.bfloat16))


def column_spectrum(rows_re, rows_im, cos_part, sin_part):
    spec_re = jnp.einsum("tjr,ri->tji", rows_re, cos_part, preferred_element_type=jnp.float32)
    spec_re = spec_re + jnp.einsum(
        "tjr,ri->tji", rows_im, sin_part, preferred_element_type=jnp.float32
    )
    spec_im = jnp.einsum("tjr,ri->tji", rows_im, cos_part, preferred_element_type=jnp.float32)
    spec_im = spec_im - jnp.einsum(
        "tjr,ri->tji", rows_re, sin_part, preferred_element_type=jnp.float32
    )
    return (spec_re, spec_im)


def local(mask, kernels, kernel_weights):
    tiles_here, rows, pixels = mask.shape
    count = kernels.shape[4]
    conds, kerns = kernel_weights.shape
    items = conds * kerns
    cos_table, sin_table = tables(pixels, count)
    row_re = jnp.einsum("trc,cj->tjr", mask, cos_table, preferred_element_type=jnp.float32).astype(
        jnp.bfloat16
    )
    row_im = (
        -jnp.einsum("trc,cj->tjr", mask, sin_table, preferred_element_type=jnp.float32)
    ).astype(jnp.bfloat16)
    cols_re, cols_im = (
        lax.all_to_all(row_re, "tile", split_axis=1, concat_axis=2, tiled=True),
        lax.all_to_all(row_im, "tile", split_axis=1, concat_axis=2, tiled=True),
    )
    spec_re, spec_im = column_spectrum(cols_re, cols_im, cos_table, sin_table)
    freq_here = kernels.shape[3]
    kern_re = kernels[0].reshape(items, freq_here, count)
    kern_im = kernels[1].reshape(items, freq_here, count)
    filt_re, filt_im = filter_spectrum(spec_re, spec_im, kern_re, kern_im)
    half_re, half_im = half_transform(filt_re, filt_im, cos_table, sin_table)
    power = field_power(
        lax.all_to_all(half_re, "tile", split_axis=3, concat_axis=2, tiled=True),
        lax.all_to_all(half_im, "tile", split_axis=3, concat_axis=2, tiled=True),
        cos_table,
        sin_table,
    )
    power = power.reshape(tiles_here, conds, kerns, rows, pixels)
    weighted = jnp.einsum("tckrp,ck->tcrp", power, kernel_weights, precision=lax.Precision.HIGHEST)
    intensity = lax.psum_scatter(weighted, "kern", scatter_dimension=3, tiled=True)
    local_low = jnp.min(intensity, axis=1)
    local_high = jnp.max(intensity, axis=1)
    low = lax.pmin(local_low, "cond")
    high = lax.pmax(local_high, "cond")
    return (low, high)


def host_tables(length, count):
    pixel = np.arange(length, dtype=np.int64)[:, None]
    freq = np.arange(count, dtype=np.int64)[None, :] - count // 2
    phase = np.mod(pixel * freq, length).astype(np.float64) * (2.0 * math.pi / length)
    factor = 1.0 / math.sqrt(length)
    return np.cos(phase) * factor, np.sin(phase) * factor


MESH = pl.DeviceIdType.MESH


def fused_kernel(sizes, mask_ref, weight_ref, wave_hbm, kern_hbm, out_ref, *scratch):
    tile, kern, cond = sizes
    (wave, held, row_send, cols, spec, filt, recv, turn, back, half, grid, power, cross, pairs) = scratch[:14]
    (quarter_send, quarter_recv, plane_send, plane_recv, final) = scratch[14:19]
    (load_sem, row_out, row_in, pair_out, pair_in, send_out, send_in, pass_out, pass_in) = scratch[19:28]
    (quarter_out, quarter_in, plane_out, plane_in, final_out, final_in) = scratch[28:]
    rows, pixels = mask_ref.shape
    _, conds, kerns, freqs, count = kern_hbm.shape
    planes = conds * cond
    width = tile // planes
    items = kerns // width
    part = freqs // cond
    wide = back.shape[1] // 2
    lanes = pixels // 2
    side = lanes // width
    steps = back.shape[0]
    chunk = plane_recv.shape[2]
    subs = plane_recv.shape[1]
    me = lax.axis_index("tile")
    line = lax.axis_index("kern")
    core = lax.axis_index("cond")
    plane = lax.div(me, width)
    column = lax.rem(me, width)
    source = lax.div(plane, conds)

    def remote(src, dst, out_sem, in_sem, to_tile, to_line, to_core):
        return pltpu.make_async_remote_copy(
            src_ref=src,
            dst_ref=dst,
            send_sem=out_sem,
            recv_sem=in_sem,
            device_id={"tile": to_tile, "kern": to_line, "cond": to_core},
            device_id_type=MESH,
        )

    def arrived(ref, sem):
        pltpu.make_async_copy(ref, ref, sem).wait()

    wave_load = pltpu.make_async_copy(wave_hbm, wave, load_sem.at[0])
    kern_load = pltpu.make_async_copy(kern_hbm, held, load_sem.at[1])
    wave_load.start()
    kern_load.start()

    barrier = pltpu.get_barrier_semaphore()
    for step in range(tile - 1, 0, -1):
        for flip in range(cond):
            pl.semaphore_signal(
                barrier,
                inc=1,
                device_id={
                    "tile": lax.rem(me + step, tile),
                    "kern": line,
                    "cond": lax.rem(core + flip, cond),
                },
                device_id_type=MESH,
            )
    pl.semaphore_signal(
        barrier, inc=1, device_id={"tile": me, "kern": line, "cond": 1 - core}, device_id_type=MESH
    )
    for shift in range(width):
        pl.semaphore_signal(
            barrier,
            inc=1,
            device_id={
                "tile": plane * width + lax.rem(column + shift, width),
                "kern": 1 - line,
                "cond": core,
            },
            device_id_type=MESH,
        )
    greeted = (tile - 1) * cond + 1 + width

    wave_load.wait()
    row = jnp.dot(mask_ref[...], wave[...], preferred_element_type=jnp.float32).T
    row_send[:, :freqs, :] = row[:count].reshape(tile, freqs, rows).astype(jnp.bfloat16)
    row_send[:, freqs:, :] = (-row[count:]).reshape(tile, freqs, rows).astype(jnp.bfloat16)

    pl.semaphore_wait(barrier, greeted)
    place = cols.at[:, pl.ds(pl.multiple_of(me * rows, rows), rows)]
    pltpu.make_async_copy(row_send.at[me], place, row_in.at[me]).start()
    for step in range(tile - 1, 0, -1):
        to = lax.rem(me + step, tile)
        remote(
            row_send.at[to], place, row_out.at[step], row_in.at[me], to, line, core
        ).start()
    pair_copy = remote(
        weight_ref, pairs, pair_out.at[0], pair_in.at[0], me, line, 1 - core
    )
    pair_copy.start()

    for shift in range(width):
        for layer in range(planes // cond):
            at = pl.multiple_of(
                ((core * (planes // cond) + layer) * width + shift) * rows, rows
            )
            to = (shift * (planes // cond) + layer) * rows
            block = wave[pl.ds(at, rows), :].astype(jnp.float32).T.astype(jnp.bfloat16)
            turn[:count, to : to + rows] = block[:count]
            turn[:count, lanes + to : lanes + to + rows] = block[count:]
            turn[count:, to : to + rows] = -block[count:]
            turn[count:, lanes + to : lanes + to + rows] = block[:count]
    for step in range(steps):
        back[step, :wide, :] = wave[step * wide : (step + 1) * wide, :count]
        back[step, wide:, :] = wave[step * wide : (step + 1) * wide, count:]
    pack = 16
    first = lax.broadcasted_iota(jnp.int32, (pack, count), 0) == 0
    middle = jnp.broadcast_to(
        wave[pixels // 2 : pixels // 2 + pack, :count].astype(jnp.float32)[:1], (pack, count)
    )
    back[0, wide : wide + pack, :] = jnp.where(
        first, middle, wave[:pack, count:].astype(jnp.float32)
    ).astype(jnp.bfloat16)
    power[...] = jnp.zeros_like(power)
    cross[...] = jnp.zeros_like(cross)

    for step in range(tile):
        to = lax.rem(me + step, tile)
        arrived(cols.at[:, pl.ds(pl.multiple_of(to * rows, rows), rows)], row_in.at[to])
    mixed = jnp.dot(cols[...], wave[...], preferred_element_type=jnp.float32)
    spec[0] = mixed[:freqs, :count] + mixed[freqs:, count:]
    spec[1] = mixed[freqs:, :count] - mixed[:freqs, count:]
    kern_load.wait()

    def targets():
        for layer in range(conds):
            for shift in range(width):
                for other in range(cond):
                    index = (layer * width + shift) * cond + other
                    to = (core * conds + layer) * width + shift
                    yield index, layer, shift, other, to, jnp.logical_and(to == me, other == core)

    def filter_item(item):
        for layer in range(conds):
            for shift in range(width):
                slot = shift * items + item
                for at in range(0, freqs, pack):
                    near = pl.ds(at, pack)
                    kern_re = held[0, layer, slot, near, :].astype(jnp.float32)
                    kern_im = held[1, layer, slot, near, :].astype(jnp.float32)
                    spec_re = spec[0, near, :]
                    spec_im = spec[1, near, :]
                    filt[layer, slot, near, :count] = (
                        spec_re * kern_re - spec_im * kern_im
                    ).astype(jnp.bfloat16)
                    filt[layer, slot, near, count:] = (
                        spec_re * kern_im + spec_im * kern_re
                    ).astype(jnp.bfloat16)

    def send_item(item):
        for index, layer, shift, other, to, mine in targets():
            src = filt.at[layer, shift * items + item, pl.ds(other * part, part)]
            dst = recv.at[item, me, pl.ds(other * part, part)]

            @pl.when(mine)
            def _():
                pltpu.make_async_copy(src, dst, send_in.at[item, me]).start()

            @pl.when(jnp.logical_not(mine))
            def _():
                remote(
                    src, dst, send_out.at[item, index], send_in.at[item, me], to, line, other
                ).start()

    filter_item(0)

    def source_step(item, carry):
        filter_item(item)
        send_item(item - 1)
        return carry

    lax.fori_loop(1, items, source_step, 0)
    send_item(items - 1)

    pair_copy.wait()
    weights = jnp.where(source == core, weight_ref[...], pairs[...])
    lane = lax.broadcasted_iota(jnp.int32, weights.shape, 1)
    level = lax.broadcasted_iota(jnp.int32, weights.shape, 0)
    weights = jnp.where(level == lax.rem(plane, conds), weights, 0.0)
    sign = jnp.where(line == 0, 2.0, -2.0)
    mine_half = pl.ds(pl.multiple_of(core * part, part), part)
    their_half = pl.ds(pl.multiple_of((1 - core) * part, part), part)

    def passed(item, origin):
        return remote(
            recv.at[item, origin, mine_half],
            recv.at[item, origin, mine_half],
            pass_out.at[item, origin],
            pass_in.at[item, origin],
            me,
            line,
            1 - core,
        )

    peers = []
    for turn_x in range(width):
        for turn_y in range(kern):
            if turn_x or turn_y:
                peers.append((turn_x, turn_y))

    def quarter(index, piece):
        turn_x, turn_y = peers[index]
        to_column = lax.rem(column + turn_x, width)
        to_line = lax.rem(line + turn_y, kern)
        span = pl.ds(piece * chunk, chunk)
        return remote(
            quarter_send.at[to_line, to_column, span],
            quarter_recv.at[index, span],
            quarter_out.at[piece, index],
            quarter_in.at[piece, index],
            plane * width + to_column,
            to_line,
            core,
        )

    def item_step(item, carry):
        for origin in range(tile):
            arrived(recv.at[item, origin, mine_half], send_in.at[item, origin])
            passed(item, origin).start()
        for origin in range(tile):
            arrived(recv.at[item, origin, their_half], pass_in.at[item, origin])
        half[...] = jnp.dot(
            recv[item].reshape(count, 2 * count), turn[...], preferred_element_type=jnp.float32
        ).astype(jnp.bfloat16)
        weight = jnp.sum(jnp.where(lane == column * items + item, weights, 0.0))

        def pixel_step(step, carry):
            grid[...] = jnp.dot(back[step], half[...], preferred_element_type=jnp.float32)

            def group(at, carry):
                near = pl.ds(pl.multiple_of(at * pack, pack), pack)
                far = pl.ds(pl.multiple_of(wide + at * pack, pack), pack)
                a_re = grid[near, :lanes]
                a_im = grid[near, lanes:]
                b_re = grid[far, :lanes]
                b_im = grid[far, lanes:]
                into = pl.ds(pl.multiple_of(step * wide + at * pack, pack), pack)
                power[into, :] += weight * (
                    (a_re * a_re + a_im * a_im) + (b_re * b_re + b_im * b_im)
                )
                cross[into, :] += weight * (a_im * b_re - a_re * b_im)
                return carry

            lax.fori_loop(0, wide // pack, group, 0)

            @pl.when(step == 0)
            def _():
                top = 8
                a_re = grid[:top, :lanes]
                a_im = grid[:top, lanes:]
                b_re = grid[wide : wide + top, :lanes]
                b_im = grid[wide : wide + top, lanes:]
                a = a_re * a_re + a_im * a_im
                b = b_re * b_re + b_im * b_im
                only = lax.broadcasted_iota(jnp.int32, (top, lanes), 0) == 0
                power[:top, :] -= jnp.where(only, (0.5 * weight) * (a + b), 0.0)
                cross[:top, :] += jnp.where(
                    only, weight * (0.25 * (a - b) - (a_im * b_re - a_re * b_im)), 0.0
                )

            @pl.when(item == items - 1)
            def _():
                for piece in range(wide // chunk):

                    def finish(at, carry):
                        into = pl.ds(
                            pl.multiple_of(step * wide + piece * chunk + at * pack, pack), pack
                        )
                        total = power[into, :]
                        twice = 2.0 * cross[into, :]
                        for shift in range(width):
                            own = slice(shift * side, (shift + 1) * side)
                            quarter_send[0, shift, into, :] = (
                                total[:, own] + twice[:, own]
                            ).astype(jnp.bfloat16)
                            quarter_send[1, shift, into, :] = (
                                total[:, own] - twice[:, own]
                            ).astype(jnp.bfloat16)
                        return carry

                    lax.fori_loop(0, chunk // pack, finish, 0)
                    for index in range(len(peers)):
                        quarter(index, step * (wide // chunk) + piece).start()

            return carry

        lax.fori_loop(0, steps, pixel_step, 0)
        return carry

    lax.fori_loop(0, items, item_step, 0)

    def to_plane(layer, piece):
        other = piece // subs
        return (
            plane_send.at[layer, pl.ds(piece * chunk, chunk)],
            plane_recv.at[plane, piece % subs],
            plane_out.at[layer, piece],
            plane_in.at[plane, piece % subs],
            (core * (planes // cond) + layer) * width + column,
            line,
            other,
        )

    def own_plane(layer, piece):
        return jnp.logical_and(
            core * (planes // cond) + layer == plane, piece // subs == core
        )

    pieces = subs * cond
    own_side = pl.ds(pl.multiple_of(column * side, side), side)
    for piece in range(pieces):
        for index in range(len(peers)):
            arrived(quarter_recv.at[index, pl.ds(piece * chunk, chunk)], quarter_in.at[piece, index])
        for at in range(piece * chunk, (piece + 1) * chunk, pack):
            span = pl.ds(at, pack)
            total = power[span, own_side] + sign * cross[span, own_side]
            for index in range(len(peers)):
                total = total + quarter_recv[index, span, :].astype(jnp.float32)
            for layer in range(planes // cond):
                plane_send[layer, span, :] = total[:, layer * rows : (layer + 1) * rows].astype(
                    jnp.bfloat16
                )
        for layer in range(planes // cond):
            src, dst, out_sem, in_sem, to, to_line, other = to_plane(layer, piece)

            @pl.when(own_plane(layer, piece))
            def _():
                pltpu.make_async_copy(src, dst, in_sem).start()

            @pl.when(jnp.logical_not(own_plane(layer, piece)))
            def _():
                remote(src, dst, out_sem, in_sem, to, to_line, other).start()

    def swap(sub):
        span = pl.ds(pl.multiple_of((core * subs + sub) * chunk, chunk), chunk)
        return remote(
            final.at[:, span], final.at[:, span], final_out.at[sub], final_in.at[sub], me, line, 1 - core
        )

    for sub in range(subs):
        for layer in range(planes):
            arrived(plane_recv.at[layer, sub], plane_in.at[layer, sub])
        for at in range(0, chunk, pack):
            values = [
                plane_recv[layer, sub, at : at + pack, :].astype(jnp.float32)
                for layer in range(planes)
            ]
            into = pl.ds(pl.multiple_of((core * subs + sub) * chunk + at, pack), pack)
            final[0, into, :] = functools.reduce(jnp.minimum, values)
            final[1, into, :] = functools.reduce(jnp.maximum, values)
        swap(sub).start()

    for step in range(1, tile):
        to = lax.rem(me + step, tile)
        pltpu.make_async_copy(row_send.at[to], row_send.at[to], row_out.at[step]).wait()

    def drain(item, carry):
        for index, layer, shift, other, to, mine in targets():
            src = filt.at[layer, shift * items + item, pl.ds(other * part, part)]

            @pl.when(jnp.logical_not(mine))
            def _():
                arrived(src, send_out.at[item, index])

        for origin in range(tile):
            arrived(recv.at[item, origin, mine_half], pass_out.at[item, origin])
        return carry

    lax.fori_loop(0, items, drain, 0)
    for piece in range(pieces):
        for index in range(len(peers)):
            quarter(index, piece).wait_send()
        for layer in range(planes // cond):

            @pl.when(jnp.logical_not(own_plane(layer, piece)))
            def _():
                arrived(plane_send.at[layer, pl.ds(piece * chunk, chunk)], plane_out.at[layer, piece])

    for sub in range(subs):
        their = pl.ds(pl.multiple_of(((1 - core) * subs + sub) * chunk, chunk), chunk)
        arrived(final.at[:, their], final_in.at[sub])
        swap(sub).wait_send()
    out_ref[...] = final[...]


def fused(sizes, mask, kernels, weights, wave):
    tile, kern, cond = sizes
    rows, pixels = mask.shape
    _, conds, kerns, freqs, count = kernels.shape
    planes = conds * cond
    width = tile // planes
    items = kerns // width
    lanes = pixels // 2
    wide = 256
    chunk = 128
    steps = lanes // wide
    pieces = lanes // chunk
    peers = width * kern - 1
    dma = pltpu.SemaphoreType.DMA
    return pl.pallas_call(
        functools.partial(fused_kernel, sizes),
        out_shape=jax.ShapeDtypeStruct((2, lanes, rows), jnp.float32),
        in_specs=[
            pl.BlockSpec(memory_space=pltpu.VMEM),
            pl.BlockSpec(memory_space=pltpu.VMEM),
            pl.BlockSpec(memory_space=pl.ANY),
            pl.BlockSpec(memory_space=pl.ANY),
        ],
        out_specs=pl.BlockSpec(memory_space=pltpu.VMEM),
        scratch_shapes=[
            pltpu.VMEM((pixels, 2 * count), jnp.bfloat16),
            pltpu.VMEM(kernels.shape, jnp.bfloat16),
            pltpu.VMEM((tile, 2 * freqs, rows), jnp.bfloat16),
            pltpu.VMEM((2 * freqs, pixels), jnp.bfloat16),
            pltpu.VMEM((2, freqs, count), jnp.float32),
            pltpu.VMEM((conds, kerns, freqs, 2 * count), jnp.bfloat16),
            pltpu.VMEM((items, tile, freqs, 2 * count), jnp.bfloat16),
            pltpu.VMEM((2 * count, pixels), jnp.bfloat16),
            pltpu.VMEM((steps, 2 * wide, count), jnp.bfloat16),
            pltpu.VMEM((count, pixels), jnp.bfloat16),
            pltpu.VMEM((2 * wide, pixels), jnp.float32),
            pltpu.VMEM((lanes, lanes), jnp.float32),
            pltpu.VMEM((lanes, lanes), jnp.float32),
            pltpu.VMEM(weights.shape, jnp.float32),
            pltpu.VMEM((kern, width, lanes, lanes // width), jnp.bfloat16),
            pltpu.VMEM((peers, lanes, lanes // width), jnp.bfloat16),
            pltpu.VMEM((planes // cond, lanes, rows), jnp.bfloat16),
            pltpu.VMEM((planes, pieces // cond, chunk, rows), jnp.bfloat16),
            pltpu.VMEM((2, lanes, rows), jnp.float32),
            dma((2,)),
            dma((tile,)),
            dma((tile,)),
            dma((1,)),
            dma((1,)),
            dma((items, tile)),
            dma((items, tile)),
            dma((items, tile)),
            dma((items, tile)),
            dma((pieces, peers)),
            dma((pieces, peers)),
            dma((planes // cond, pieces)),
            dma((planes, pieces // cond)),
            dma((pieces // cond,)),
            dma((pieces // cond,)),
        ],
        compiler_params=pltpu.CompilerParams(
            collective_id=0, has_side_effects=True, vmem_limit_bytes=60 * 1024 * 1024
        ),
    )(mask, weights, wave, kernels)


def place_kernel(final_ref, low_ref, high_ref):
    line = lax.axis_index("kern")
    size = final_ref.shape[1]
    slot = lax.broadcasted_iota(jnp.int32, (size, size), 0)
    pixel = lax.broadcasted_iota(jnp.int32, (size, size), 1)
    wanted = jnp.where(line == 0, pixel, jnp.where(pixel == 0, 0, size - pixel))
    order = (slot == wanted).astype(jnp.float32)
    for ref, index in ((low_ref, 0), (high_ref, 1)):
        ref[0] = lax.dot_general(
            final_ref[index],
            order,
            (((0,), (0,)), ((), ())),
            preferred_element_type=jnp.float32,
            precision=lax.Precision.HIGHEST,
        )


def planes_of(sizes, mask, kernels, kernel_weights):
    _, rows, pixels = mask.shape
    count = kernels.shape[4]
    conds, kerns = kernel_weights.shape
    cos, sin = host_tables(pixels, count)
    wave = jnp.asarray(np.concatenate([cos, sin], axis=1), jnp.bfloat16)
    weights = jnp.pad(kernel_weights, ((0, 8 - conds), (0, 128 - kerns)))
    final = fused(sizes, mask[0], kernels, weights, wave)
    shape = jax.ShapeDtypeStruct((1, rows, pixels // 2), jnp.float32)
    return pl.pallas_call(place_kernel, out_shape=(shape, shape))(final)


def plan(mesh):
    tile, kern, cond = (mesh.shape[name] for name in ("tile", "kern", "cond"))

    def body(mask, kernels, kernel_weights):
        conds, kerns = kernel_weights.shape
        freqs, count = kernels.shape[3:]
        rows, pixels = mask.shape[1:]
        split = kern == 2 and cond == 2 and conds == 2 and tile == 2 * conds * cond
        split = split and mask.shape[0] == 1 and count * 2 == pixels and kerns % 2 == 0
        split = split and rows == 128 and freqs % 32 == 0 and pixels == tile * rows
        if split and kerns <= 128 and count % 512 == 0:
            return planes_of((tile, kern, cond), mask, kernels, kernel_weights)
        return local(mask, kernels, kernel_weights)

    return body


def solution(mesh):
    placed = (P(None, "tile", None), P(None, "cond", "kern", "tile", None), P("cond", "kern"))
    return jax.shard_map(
        plan(mesh),
        mesh=mesh,
        in_specs=placed,
        out_specs=(P(None, "tile", "kern"), P(None, "tile", "kern")),
        check_vma=False,
    )
```

```python
import functools
import math

import jax
import jax.numpy as jnp
import numpy as np
from jax import lax
from jax.experimental import pallas as pl
from jax.experimental.pallas import tpu as pltpu
from jax.sharding import PartitionSpec as P


def tables(length, count):
    pixel = jnp.arange(length, dtype=jnp.int32)[:, None]
    freq = jnp.arange(count, dtype=jnp.int32)[None, :] - count // 2
    phase = jnp.mod(pixel * freq, length).astype(jnp.float32) * (2.0 * math.pi / length)
    factor = 1.0 / math.sqrt(length)
    return (
        (jnp.cos(phase) * factor).astype(jnp.bfloat16),
        (jnp.sin(phase) * factor).astype(jnp.bfloat16),
    )


def field_power(half_re, half_im, cos_table, sin_table):
    field_re = jnp.einsum("tnjr,pj->tnrp", half_re, cos_table, preferred_element_type=jnp.float32)
    field_re = field_re - jnp.einsum(
        "tnjr,pj->tnrp", half_im, sin_table, preferred_element_type=jnp.float32
    )
    field_im = jnp.einsum("tnjr,pj->tnrp", half_re, sin_table, preferred_element_type=jnp.float32)
    field_im = field_im + jnp.einsum(
        "tnjr,pj->tnrp", half_im, cos_table, preferred_element_type=jnp.float32
    )
    return field_re * field_re + field_im * field_im


def filter_spectrum(spec_re, spec_im, kern_re, kern_im):
    kern_re = kern_re.astype(jnp.float32)
    kern_im = kern_im.astype(jnp.float32)
    filt_re = spec_re[:, None] * kern_re[None] - spec_im[:, None] * kern_im[None]
    filt_im = spec_re[:, None] * kern_im[None] + spec_im[:, None] * kern_re[None]
    return (filt_re.astype(jnp.bfloat16), filt_im.astype(jnp.bfloat16))


def half_transform(filt_re, filt_im, cos_part, sin_part):
    half_re = jnp.einsum("tnji,ri->tnjr", filt_re, cos_part, preferred_element_type=jnp.float32)
    half_re = half_re - jnp.einsum(
        "tnji,ri->tnjr", filt_im, sin_part, preferred_element_type=jnp.float32
    )
    half_im = jnp.einsum("tnji,ri->tnjr", filt_re, sin_part, preferred_element_type=jnp.float32)
    half_im = half_im + jnp.einsum(
        "tnji,ri->tnjr", filt_im, cos_part, preferred_element_type=jnp.float32
    )
    return (half_re.astype(jnp.bfloat16), half_im.astype(jnp.bfloat16))


def column_spectrum(rows_re, rows_im, cos_part, sin_part):
    spec_re = jnp.einsum("tjr,ri->tji", rows_re, cos_part, preferred_element_type=jnp.float32)
    spec_re = spec_re + jnp.einsum(
        "tjr,ri->tji", rows_im, sin_part, preferred_element_type=jnp.float32
    )
    spec_im = jnp.einsum("tjr,ri->tji", rows_im, cos_part, preferred_element_type=jnp.float32)
    spec_im = spec_im - jnp.einsum(
        "tjr,ri->tji", rows_re, sin_part, preferred_element_type=jnp.float32
    )
    return (spec_re, spec_im)


def local(mask, kernels, kernel_weights):
    tiles_here, rows, pixels = mask.shape
    count = kernels.shape[4]
    conds, kerns = kernel_weights.shape
    items = conds * kerns
    cos_table, sin_table = tables(pixels, count)
    row_re = jnp.einsum("trc,cj->tjr", mask, cos_table, preferred_element_type=jnp.float32).astype(
        jnp.bfloat16
    )
    row_im = (
        -jnp.einsum("trc,cj->tjr", mask, sin_table, preferred_element_type=jnp.float32)
    ).astype(jnp.bfloat16)
    cols_re, cols_im = (
        lax.all_to_all(row_re, "tile", split_axis=1, concat_axis=2, tiled=True),
        lax.all_to_all(row_im, "tile", split_axis=1, concat_axis=2, tiled=True),
    )
    spec_re, spec_im = column_spectrum(cols_re, cols_im, cos_table, sin_table)
    freq_here = kernels.shape[3]
    kern_re = kernels[0].reshape(items, freq_here, count)
    kern_im = kernels[1].reshape(items, freq_here, count)
    filt_re, filt_im = filter_spectrum(spec_re, spec_im, kern_re, kern_im)
    half_re, half_im = half_transform(filt_re, filt_im, cos_table, sin_table)
    power = field_power(
        lax.all_to_all(half_re, "tile", split_axis=3, concat_axis=2, tiled=True),
        lax.all_to_all(half_im, "tile", split_axis=3, concat_axis=2, tiled=True),
        cos_table,
        sin_table,
    )
    power = power.reshape(tiles_here, conds, kerns, rows, pixels)
    weighted = jnp.einsum("tckrp,ck->tcrp", power, kernel_weights, precision=lax.Precision.HIGHEST)
    intensity = lax.psum_scatter(weighted, "kern", scatter_dimension=3, tiled=True)
    local_low = jnp.min(intensity, axis=1)
    local_high = jnp.max(intensity, axis=1)
    low = lax.pmin(local_low, "cond")
    high = lax.pmax(local_high, "cond")
    return (low, high)


def host_tables(length, count):
    pixel = np.arange(length, dtype=np.int64)[:, None]
    freq = np.arange(count, dtype=np.int64)[None, :] - count // 2
    phase = np.mod(pixel * freq, length).astype(np.float64) * (2.0 * math.pi / length)
    factor = 1.0 / math.sqrt(length)
    return np.cos(phase) * factor, np.sin(phase) * factor


MESH = pl.DeviceIdType.MESH


def fused_kernel(sizes, mask_ref, weight_ref, wave_hbm, kern_hbm, out_ref, *scratch):
    tile, kern, cond = sizes
    (wave, held, row_send, cols, spec, filt, recv, turn, back, half, grid, power, cross, pairs) = scratch[:14]
    (quarter_send, quarter_recv, plane_send, plane_recv, final) = scratch[14:19]
    weight = scratch[-1]
    (load_sem, row_out, row_in, pair_out, pair_in, send_out, send_in, pass_out, pass_in) = scratch[19:28]
    (quarter_out, quarter_in, plane_out, plane_in, final_out, final_in, share_out, share_in) = (
        scratch[28:-1]
    )
    rows, pixels = mask_ref.shape
    _, conds, kerns, freqs, count = kern_hbm.shape
    planes = conds * cond
    width = tile // planes
    items = kerns // width
    part = freqs // cond
    wide = back.shape[1] // 2
    lanes = pixels // 2
    side = lanes // width
    steps = back.shape[0]
    chunk = plane_recv.shape[2]
    subs = plane_recv.shape[1]
    me = lax.axis_index("tile")
    line = lax.axis_index("kern")
    core = lax.axis_index("cond")
    plane = lax.div(me, width)
    column = lax.rem(me, width)
    source = lax.div(plane, conds)

    def remote(src, dst, out_sem, in_sem, to_tile, to_line, to_core):
        return pltpu.make_async_remote_copy(
            src_ref=src,
            dst_ref=dst,
            send_sem=out_sem,
            recv_sem=in_sem,
            device_id={"tile": to_tile, "kern": to_line, "cond": to_core},
            device_id_type=MESH,
        )

    def arrived(ref, sem):
        pltpu.make_async_copy(ref, ref, sem).wait()

    wave_load = pltpu.make_async_copy(wave_hbm, wave, load_sem.at[0])
    kern_load = pltpu.make_async_copy(kern_hbm, held, load_sem.at[1])
    wave_load.start()
    kern_load.start()

    barrier = pltpu.get_barrier_semaphore()
    for step in range(tile - 1, 0, -1):
        for flip in range(cond):
            pl.semaphore_signal(
                barrier,
                inc=1,
                device_id={
                    "tile": lax.rem(me + step, tile),
                    "kern": line,
                    "cond": lax.rem(core + flip, cond),
                },
                device_id_type=MESH,
            )
    pl.semaphore_signal(
        barrier, inc=1, device_id={"tile": me, "kern": line, "cond": 1 - core}, device_id_type=MESH
    )
    for shift in range(width):
        pl.semaphore_signal(
            barrier,
            inc=1,
            device_id={
                "tile": plane * width + lax.rem(column + shift, width),
                "kern": 1 - line,
                "cond": core,
            },
            device_id_type=MESH,
        )
    greeted = (tile - 1) * cond + 1 + width

    weight[...] = jnp.zeros_like(weight)
    weight[:conds, :kerns] = weight_ref[...]
    wave_load.wait()
    row = jnp.dot(mask_ref[...], wave[...], preferred_element_type=jnp.float32).T
    row_re = row[:count].reshape(tile, cond, part, rows).astype(jnp.bfloat16)
    row_im = (-row[count:]).reshape(tile, cond, part, rows).astype(jnp.bfloat16)
    row_send[:, :, :part, :] = row_re
    row_send[:, :, part:, :] = row_im

    pl.semaphore_wait(barrier, greeted)

    def column_of(origin, side_of):
        return cols.at[side_of, :, pl.ds(pl.multiple_of(origin * rows, rows), rows)]

    def shared(origin):
        return remote(
            column_of(origin, core),
            column_of(origin, core),
            share_out.at[origin],
            share_in.at[origin],
            me,
            line,
            1 - core,
        )

    place = column_of(me, core)
    pltpu.make_async_copy(row_send.at[me, core], place, row_in.at[me]).start()
    for step in range(tile - 1, 0, -1):
        to = lax.rem(me + step, tile)
        remote(
            row_send.at[to, core], place, row_out.at[step], row_in.at[me], to, line, core
        ).start()
    pair_copy = remote(
        weight, pairs, pair_out.at[0], pair_in.at[0], me, line, 1 - core
    )
    pair_copy.start()

    for shift in range(width):
        for layer in range(planes // cond):
            at = pl.multiple_of(
                ((core * (planes // cond) + layer) * width + shift) * rows, rows
            )
            to = (shift * (planes // cond) + layer) * rows
            block = wave[pl.ds(at, rows), :].astype(jnp.float32).T.astype(jnp.bfloat16)
            turn[:count, to : to + rows] = block[:count]
            turn[:count, lanes + to : lanes + to + rows] = block[count:]
            turn[count:, to : to + rows] = -block[count:]
            turn[count:, lanes + to : lanes + to + rows] = block[:count]
    for step in range(steps):
        back[step, :wide, :] = wave[step * wide : (step + 1) * wide, :count]
        back[step, wide:, :] = wave[step * wide : (step + 1) * wide, count:]
    pack = 16
    first = lax.broadcasted_iota(jnp.int32, (pack, count), 0) == 0
    middle = jnp.broadcast_to(
        wave[pixels // 2 : pixels // 2 + pack, :count].astype(jnp.float32)[:1], (pack, count)
    )
    back[0, wide : wide + pack, :] = jnp.where(
        first, middle, wave[:pack, count:].astype(jnp.float32)
    ).astype(jnp.bfloat16)
    power[...] = jnp.zeros_like(power)
    cross[...] = jnp.zeros_like(cross)

    order = (
        plane,
        plane + 1 - 2 * lax.rem(plane, 2),
        lax.rem(plane + planes // 2, planes),
        planes - 1 - plane,
    )
    nearest = [at * width + shift for at in order for shift in range(width)]
    for origin in nearest:
        arrived(column_of(origin, core), row_in.at[origin])
        shared(origin).start()
    for origin in nearest:
        arrived(column_of(origin, 1 - core), share_in.at[origin])
    mixed = jnp.dot(
        cols[...].reshape(2 * freqs, pixels), wave[...], preferred_element_type=jnp.float32
    )
    for other in range(cond):
        re = mixed[2 * other * part : (2 * other + 1) * part]
        im = mixed[(2 * other + 1) * part : (2 * other + 2) * part]
        spec[0, other * part : (other + 1) * part] = re[:, :count] + im[:, count:]
        spec[1, other * part : (other + 1) * part] = im[:, :count] - re[:, count:]
    kern_load.wait()

    blocks = [(layer, shift) for layer in range(conds) for shift in range(width)]

    def targets(layer, shift):
        to = (core * conds + layer) * width + shift
        for other in range(cond):
            index = (layer * width + shift) * cond + other
            yield index, other, to, jnp.logical_and(to == me, other == core)

    def filter_block(item, layer, shift):
        slot = shift * items + item
        for at in range(0, freqs, pack):
            near = pl.ds(at, pack)
            kern_re = held[0, layer, slot, near, :].astype(jnp.float32)
            kern_im = held[1, layer, slot, near, :].astype(jnp.float32)
            spec_re = spec[0, near, :]
            spec_im = spec[1, near, :]
            filt[layer, slot, near, :count] = (spec_re * kern_re - spec_im * kern_im).astype(
                jnp.bfloat16
            )
            filt[layer, slot, near, count:] = (spec_re * kern_im + spec_im * kern_re).astype(
                jnp.bfloat16
            )

    def send_block(item, layer, shift):
        for index, other, to, mine in targets(layer, shift):
            src = filt.at[layer, shift * items + item, pl.ds(other * part, part)]
            dst = recv.at[item, me, pl.ds(other * part, part)]

            @pl.when(mine)
            def _():
                pltpu.make_async_copy(src, dst, send_in.at[item, me]).start()

            @pl.when(jnp.logical_not(mine))
            def _():
                remote(
                    src, dst, send_out.at[item, index], send_in.at[item, me], to, line, other
                ).start()

    def source_step(item, carry):
        for index, block in enumerate(blocks):
            filter_block(item, *block)
            if index:
                send_block(item, *blocks[index - 1])
            else:

                @pl.when(item > 0)
                def _():
                    send_block(item - 1, *blocks[-1])

        return carry

    lax.fori_loop(0, items, source_step, 0)
    send_block(items - 1, *blocks[-1])

    pair_copy.wait()
    weights = jnp.where(source == core, weight[...], pairs[...])
    lane = lax.broadcasted_iota(jnp.int32, weights.shape, 1)
    level = lax.broadcasted_iota(jnp.int32, weights.shape, 0)
    weights = jnp.where(level == lax.rem(plane, conds), weights, 0.0)
    sign = jnp.where(line == 0, 2.0, -2.0)
    mine_half = pl.ds(pl.multiple_of(core * part, part), part)
    their_half = pl.ds(pl.multiple_of((1 - core) * part, part), part)

    def passed(item, origin):
        return remote(
            recv.at[item, origin, mine_half],
            recv.at[item, origin, mine_half],
            pass_out.at[item, origin],
            pass_in.at[item, origin],
            me,
            line,
            1 - core,
        )

    peers = []
    for turn_x in range(width):
        for turn_y in range(kern):
            if turn_x or turn_y:
                peers.append((turn_x, turn_y))

    def quarter(index, piece):
        turn_x, turn_y = peers[index]
        to_column = lax.rem(column + turn_x, width)
        to_line = lax.rem(line + turn_y, kern)
        span = pl.ds(piece * chunk, chunk)
        return remote(
            quarter_send.at[to_line, to_column, span],
            quarter_recv.at[index, span],
            quarter_out.at[piece, index],
            quarter_in.at[piece, index],
            plane * width + to_column,
            to_line,
            core,
        )

    def item_step(item, carry):
        for origin in range(tile):
            arrived(recv.at[item, origin, mine_half], send_in.at[item, origin])
            passed(item, origin).start()
        for origin in range(tile):
            arrived(recv.at[item, origin, their_half], pass_in.at[item, origin])
        half[...] = jnp.dot(
            recv[item].reshape(count, 2 * count), turn[...], preferred_element_type=jnp.float32
        ).astype(jnp.bfloat16)
        scale = jnp.sum(jnp.where(lane == column * items + item, weights, 0.0))

        def pixel_step(step, carry):
            grid[...] = jnp.dot(back[step], half[...], preferred_element_type=jnp.float32)

            def group(at, carry):
                near = pl.ds(pl.multiple_of(at * pack, pack), pack)
                far = pl.ds(pl.multiple_of(wide + at * pack, pack), pack)
                a_re = grid[near, :lanes]
                a_im = grid[near, lanes:]
                b_re = grid[far, :lanes]
                b_im = grid[far, lanes:]
                into = pl.ds(pl.multiple_of(step * wide + at * pack, pack), pack)
                power[into, :] += scale * (
                    (a_re * a_re + a_im * a_im) + (b_re * b_re + b_im * b_im)
                )
                cross[into, :] += scale * (a_im * b_re - a_re * b_im)
                return carry

            lax.fori_loop(0, wide // pack, group, 0)

            @pl.when(step == 0)
            def _():
                top = 8
                a_re = grid[:top, :lanes]
                a_im = grid[:top, lanes:]
                b_re = grid[wide : wide + top, :lanes]
                b_im = grid[wide : wide + top, lanes:]
                a = a_re * a_re + a_im * a_im
                b = b_re * b_re + b_im * b_im
                only = lax.broadcasted_iota(jnp.int32, (top, lanes), 0) == 0
                power[:top, :] -= jnp.where(only, (0.5 * scale) * (a + b), 0.0)
                cross[:top, :] += jnp.where(
                    only, scale * (0.25 * (a - b) - (a_im * b_re - a_re * b_im)), 0.0
                )

            @pl.when(item == items - 1)
            def _():
                for piece in range(wide // chunk):

                    def finish(at, carry):
                        into = pl.ds(
                            pl.multiple_of(step * wide + piece * chunk + at * pack, pack), pack
                        )
                        total = power[into, :]
                        twice = 2.0 * cross[into, :]
                        for shift in range(width):
                            own = slice(shift * side, (shift + 1) * side)
                            quarter_send[0, shift, into, :] = (
                                total[:, own] + twice[:, own]
                            ).astype(jnp.bfloat16)
                            quarter_send[1, shift, into, :] = (
                                total[:, own] - twice[:, own]
                            ).astype(jnp.bfloat16)
                        return carry

                    lax.fori_loop(0, chunk // pack, finish, 0)
                    for index in range(len(peers)):
                        quarter(index, step * (wide // chunk) + piece).start()

            return carry

        lax.fori_loop(0, steps, pixel_step, 0)
        return carry

    lax.fori_loop(0, items, item_step, 0)

    def to_plane(layer, piece):
        other = piece // subs
        return (
            plane_send.at[layer, pl.ds(piece * chunk, chunk)],
            plane_recv.at[plane, piece % subs],
            plane_out.at[layer, piece],
            plane_in.at[plane, piece % subs],
            (core * (planes // cond) + layer) * width + column,
            line,
            other,
        )

    def own_plane(layer, piece):
        return jnp.logical_and(
            core * (planes // cond) + layer == plane, piece // subs == core
        )

    pieces = subs * cond
    own_side = pl.ds(pl.multiple_of(column * side, side), side)
    for piece in range(pieces):
        for index in range(len(peers)):
            arrived(quarter_recv.at[index, pl.ds(piece * chunk, chunk)], quarter_in.at[piece, index])
        for at in range(piece * chunk, (piece + 1) * chunk, pack):
            span = pl.ds(at, pack)
            total = power[span, own_side] + sign * cross[span, own_side]
            for index in range(len(peers)):
                total = total + quarter_recv[index, span, :].astype(jnp.float32)
            for layer in range(planes // cond):
                plane_send[layer, span, :] = total[:, layer * rows : (layer + 1) * rows].astype(
                    jnp.bfloat16
                )
        for layer in range(planes // cond):
            src, dst, out_sem, in_sem, to, to_line, other = to_plane(layer, piece)

            @pl.when(own_plane(layer, piece))
            def _():
                pltpu.make_async_copy(src, dst, in_sem).start()

            @pl.when(jnp.logical_not(own_plane(layer, piece)))
            def _():
                remote(src, dst, out_sem, in_sem, to, to_line, other).start()

    def swap(sub):
        span = pl.ds(pl.multiple_of((core * subs + sub) * chunk, chunk), chunk)
        return remote(
            final.at[:, span], final.at[:, span], final_out.at[sub], final_in.at[sub], me, line, 1 - core
        )

    for sub in range(subs):
        for layer in range(planes):
            arrived(plane_recv.at[layer, sub], plane_in.at[layer, sub])
        for at in range(0, chunk, pack):
            values = [
                plane_recv[layer, sub, at : at + pack, :].astype(jnp.float32)
                for layer in range(planes)
            ]
            into = pl.ds(pl.multiple_of((core * subs + sub) * chunk + at, pack), pack)
            final[0, into, :] = functools.reduce(jnp.minimum, values).astype(jnp.bfloat16)
            final[1, into, :] = functools.reduce(jnp.maximum, values).astype(jnp.bfloat16)
        swap(sub).start()

    for step in range(1, tile):
        to = lax.rem(me + step, tile)
        arrived(row_send.at[to, core], row_out.at[step])
    for origin in range(tile):
        shared(origin).wait_send()

    def drain(item, carry):
        for layer, shift in blocks:
            for index, other, to, mine in targets(layer, shift):
                src = filt.at[layer, shift * items + item, pl.ds(other * part, part)]

                @pl.when(jnp.logical_not(mine))
                def _():
                    arrived(src, send_out.at[item, index])

        for origin in range(tile):
            arrived(recv.at[item, origin, mine_half], pass_out.at[item, origin])
        return carry

    lax.fori_loop(0, items, drain, 0)
    for piece in range(pieces):
        for index in range(len(peers)):
            quarter(index, piece).wait_send()
        for layer in range(planes // cond):

            @pl.when(jnp.logical_not(own_plane(layer, piece)))
            def _():
                arrived(plane_send.at[layer, pl.ds(piece * chunk, chunk)], plane_out.at[layer, piece])

    for sub in range(subs):
        their = pl.ds(pl.multiple_of(((1 - core) * subs + sub) * chunk, chunk), chunk)
        arrived(final.at[:, their], final_in.at[sub])
        swap(sub).wait_send()
    out_ref[...] = final[...]


def fused(sizes, mask, kernels, weights, wave):
    tile, kern, cond = sizes
    rows, pixels = mask.shape
    _, conds, kerns, freqs, count = kernels.shape
    planes = conds * cond
    width = tile // planes
    items = kerns // width
    lanes = pixels // 2
    wide = 256
    chunk = 128
    steps = lanes // wide
    pieces = lanes // chunk
    peers = width * kern - 1
    dma = pltpu.SemaphoreType.DMA
    return pl.pallas_call(
        functools.partial(fused_kernel, sizes),
        out_shape=jax.ShapeDtypeStruct((2, lanes, rows), jnp.bfloat16),
        in_specs=[
            pl.BlockSpec(memory_space=pltpu.VMEM),
            pl.BlockSpec(memory_space=pltpu.VMEM),
            pl.BlockSpec(memory_space=pl.ANY),
            pl.BlockSpec(memory_space=pl.ANY),
        ],
        out_specs=pl.BlockSpec(memory_space=pltpu.VMEM),
        scratch_shapes=[
            pltpu.VMEM((pixels, 2 * count), jnp.bfloat16),
            pltpu.VMEM(kernels.shape, jnp.bfloat16),
            pltpu.VMEM((tile, cond, 2 * freqs // cond, rows), jnp.bfloat16),
            pltpu.VMEM((cond, 2 * freqs // cond, pixels), jnp.bfloat16),
            pltpu.VMEM((2, freqs, count), jnp.float32),
            pltpu.VMEM((conds, kerns, freqs, 2 * count), jnp.bfloat16),
            pltpu.VMEM((items, tile, freqs, 2 * count), jnp.bfloat16),
            pltpu.VMEM((2 * count, pixels), jnp.bfloat16),
            pltpu.VMEM((steps, 2 * wide, count), jnp.bfloat16),
            pltpu.VMEM((count, pixels), jnp.bfloat16),
            pltpu.VMEM((2 * wide, pixels), jnp.float32),
            pltpu.VMEM((lanes, lanes), jnp.float32),
            pltpu.VMEM((lanes, lanes), jnp.float32),
            pltpu.VMEM((8, 128), jnp.float32),
            pltpu.VMEM((kern, width, lanes, lanes // width), jnp.bfloat16),
            pltpu.VMEM((peers, lanes, lanes // width), jnp.bfloat16),
            pltpu.VMEM((planes // cond, lanes, rows), jnp.bfloat16),
            pltpu.VMEM((planes, pieces // cond, chunk, rows), jnp.bfloat16),
            pltpu.VMEM((2, lanes, rows), jnp.bfloat16),
            dma((2,)),
            dma((tile,)),
            dma((tile,)),
            dma((1,)),
            dma((1,)),
            dma((items, tile)),
            dma((items, tile)),
            dma((items, tile)),
            dma((items, tile)),
            dma((pieces, peers)),
            dma((pieces, peers)),
            dma((planes // cond, pieces)),
            dma((planes, pieces // cond)),
            dma((pieces // cond,)),
            dma((pieces // cond,)),
            dma((tile,)),
            dma((tile,)),
            pltpu.VMEM((8, 128), jnp.float32),
        ],
        compiler_params=pltpu.CompilerParams(
            collective_id=0, has_side_effects=True, vmem_limit_bytes=60 * 1024 * 1024
        ),
    )(mask, weights, wave, kernels)


def place_kernel(final_ref, low_ref, high_ref):
    line = lax.axis_index("kern")
    size = final_ref.shape[1]
    slot = lax.broadcasted_iota(jnp.int32, (size, size), 0)
    pixel = lax.broadcasted_iota(jnp.int32, (size, size), 1)
    wanted = jnp.where(line == 0, pixel, jnp.where(pixel == 0, 0, size - pixel))
    order = (slot == wanted).astype(jnp.bfloat16)
    for ref, index in ((low_ref, 0), (high_ref, 1)):
        ref[0] = lax.dot_general(
            final_ref[index],
            order,
            (((0,), (0,)), ((), ())),
            preferred_element_type=jnp.float32,
        )


def planes_of(sizes, mask, kernels, kernel_weights):
    _, rows, pixels = mask.shape
    count = kernels.shape[4]
    conds, kerns = kernel_weights.shape
    cos, sin = host_tables(pixels, count)
    wave = jnp.asarray(np.concatenate([cos, sin], axis=1), jnp.bfloat16)
    final = fused(sizes, mask[0], kernels, kernel_weights, wave)
    shape = jax.ShapeDtypeStruct((1, rows, pixels // 2), jnp.float32)
    return pl.pallas_call(place_kernel, out_shape=(shape, shape))(final)


def plan(mesh):
    tile, kern, cond = (mesh.shape[name] for name in ("tile", "kern", "cond"))

    def body(mask, kernels, kernel_weights):
        conds, kerns = kernel_weights.shape
        freqs, count = kernels.shape[3:]
        rows, pixels = mask.shape[1:]
        split = kern == 2 and cond == 2 and conds == 2 and tile == 2 * conds * cond
        split = split and mask.shape[0] == 1 and count * 2 == pixels and kerns % 2 == 0
        split = split and rows == 128 and freqs % 32 == 0 and pixels == tile * rows
        if split and kerns <= 128 and count % 512 == 0:
            return planes_of((tile, kern, cond), mask, kernels, kernel_weights)
        return local(mask, kernels, kernel_weights)

    return body


def solution(mesh):
    placed = (P(None, "tile", None), P(None, "cond", "kern", "tile", None), P("cond", "kern"))
    return jax.shard_map(
        plan(mesh),
        mesh=mesh,
        in_specs=placed,
        out_specs=(P(None, "tile", "kern"), P(None, "tile", "kern")),
        check_vma=False,
    )
```

```python
import functools
import math

import jax
import jax.numpy as jnp
import numpy as np
from jax import lax
from jax.experimental import pallas as pl
from jax.experimental.pallas import tpu as pltpu
from jax.sharding import PartitionSpec as P


def tables(length, count):
    pixel = jnp.arange(length, dtype=jnp.int32)[:, None]
    freq = jnp.arange(count, dtype=jnp.int32)[None, :] - count // 2
    phase = jnp.mod(pixel * freq, length).astype(jnp.float32) * (2.0 * math.pi / length)
    factor = 1.0 / math.sqrt(length)
    return (
        (jnp.cos(phase) * factor).astype(jnp.bfloat16),
        (jnp.sin(phase) * factor).astype(jnp.bfloat16),
    )


def field_power(half_re, half_im, cos_table, sin_table):
    field_re = jnp.einsum("tnjr,pj->tnrp", half_re, cos_table, preferred_element_type=jnp.float32)
    field_re = field_re - jnp.einsum(
        "tnjr,pj->tnrp", half_im, sin_table, preferred_element_type=jnp.float32
    )
    field_im = jnp.einsum("tnjr,pj->tnrp", half_re, sin_table, preferred_element_type=jnp.float32)
    field_im = field_im + jnp.einsum(
        "tnjr,pj->tnrp", half_im, cos_table, preferred_element_type=jnp.float32
    )
    return field_re * field_re + field_im * field_im


def filter_spectrum(spec_re, spec_im, kern_re, kern_im):
    kern_re = kern_re.astype(jnp.float32)
    kern_im = kern_im.astype(jnp.float32)
    filt_re = spec_re[:, None] * kern_re[None] - spec_im[:, None] * kern_im[None]
    filt_im = spec_re[:, None] * kern_im[None] + spec_im[:, None] * kern_re[None]
    return (filt_re.astype(jnp.bfloat16), filt_im.astype(jnp.bfloat16))


def half_transform(filt_re, filt_im, cos_part, sin_part):
    half_re = jnp.einsum("tnji,ri->tnjr", filt_re, cos_part, preferred_element_type=jnp.float32)
    half_re = half_re - jnp.einsum(
        "tnji,ri->tnjr", filt_im, sin_part, preferred_element_type=jnp.float32
    )
    half_im = jnp.einsum("tnji,ri->tnjr", filt_re, sin_part, preferred_element_type=jnp.float32)
    half_im = half_im + jnp.einsum(
        "tnji,ri->tnjr", filt_im, cos_part, preferred_element_type=jnp.float32
    )
    return (half_re.astype(jnp.bfloat16), half_im.astype(jnp.bfloat16))


def column_spectrum(rows_re, rows_im, cos_part, sin_part):
    spec_re = jnp.einsum("tjr,ri->tji", rows_re, cos_part, preferred_element_type=jnp.float32)
    spec_re = spec_re + jnp.einsum(
        "tjr,ri->tji", rows_im, sin_part, preferred_element_type=jnp.float32
    )
    spec_im = jnp.einsum("tjr,ri->tji", rows_im, cos_part, preferred_element_type=jnp.float32)
    spec_im = spec_im - jnp.einsum(
        "tjr,ri->tji", rows_re, sin_part, preferred_element_type=jnp.float32
    )
    return (spec_re, spec_im)


def local(mask, kernels, kernel_weights):
    tiles_here, rows, pixels = mask.shape
    count = kernels.shape[4]
    conds, kerns = kernel_weights.shape
    items = conds * kerns
    cos_table, sin_table = tables(pixels, count)
    row_re = jnp.einsum("trc,cj->tjr", mask, cos_table, preferred_element_type=jnp.float32).astype(
        jnp.bfloat16
    )
    row_im = (
        -jnp.einsum("trc,cj->tjr", mask, sin_table, preferred_element_type=jnp.float32)
    ).astype(jnp.bfloat16)
    cols_re, cols_im = (
        lax.all_to_all(row_re, "tile", split_axis=1, concat_axis=2, tiled=True),
        lax.all_to_all(row_im, "tile", split_axis=1, concat_axis=2, tiled=True),
    )
    spec_re, spec_im = column_spectrum(cols_re, cols_im, cos_table, sin_table)
    freq_here = kernels.shape[3]
    kern_re = kernels[0].reshape(items, freq_here, count)
    kern_im = kernels[1].reshape(items, freq_here, count)
    filt_re, filt_im = filter_spectrum(spec_re, spec_im, kern_re, kern_im)
    half_re, half_im = half_transform(filt_re, filt_im, cos_table, sin_table)
    power = field_power(
        lax.all_to_all(half_re, "tile", split_axis=3, concat_axis=2, tiled=True),
        lax.all_to_all(half_im, "tile", split_axis=3, concat_axis=2, tiled=True),
        cos_table,
        sin_table,
    )
    power = power.reshape(tiles_here, conds, kerns, rows, pixels)
    weighted = jnp.einsum("tckrp,ck->tcrp", power, kernel_weights, precision=lax.Precision.HIGHEST)
    intensity = lax.psum_scatter(weighted, "kern", scatter_dimension=3, tiled=True)
    local_low = jnp.min(intensity, axis=1)
    local_high = jnp.max(intensity, axis=1)
    low = lax.pmin(local_low, "cond")
    high = lax.pmax(local_high, "cond")
    return (low, high)


def host_tables(length, count):
    pixel = np.arange(length, dtype=np.int64)[:, None]
    freq = np.arange(count, dtype=np.int64)[None, :] - count // 2
    phase = np.mod(pixel * freq, length).astype(np.float64) * (2.0 * math.pi / length)
    factor = 1.0 / math.sqrt(length)
    return np.cos(phase) * factor, np.sin(phase) * factor


MESH = pl.DeviceIdType.MESH


def fused_kernel(sizes, mask_hbm, weight_hbm, wave_hbm, kern_hbm, out_ref, *scratch):
    tile, kern, cond = sizes
    (wave, held, row_send, cols, spec, filt, recv, turn, back, half, grid, power, cross, pairs) = scratch[:14]
    (quarter_send, quarter_recv, plane_send, plane_recv) = scratch[14:18]
    weight, weight_ref, mask_ref = scratch[-3:]
    (load_sem, row_out, row_in, share_out, share_in, pair_out, pair_in) = scratch[18:25]
    (send_out, send_in, pass_out, pass_in) = scratch[25:29]
    (quarter_out, quarter_in, plane_out, plane_in) = scratch[29:33]
    rows, pixels = mask_hbm.shape
    _, conds, kerns, freqs, count = kern_hbm.shape
    planes = conds * cond
    width = tile // planes
    items = kerns // width
    part = freqs // cond
    wide = back.shape[1] // 2
    lanes = pixels // 2
    side = lanes // width
    steps = back.shape[0]
    chunk = plane_recv.shape[2]
    pieces = plane_recv.shape[1]
    me = lax.axis_index("tile")
    line = lax.axis_index("kern")
    core = lax.axis_index("cond")
    plane = lax.div(me, width)
    column = lax.rem(me, width)
    source = lax.div(plane, conds)

    def remote(src, dst, out_sem, in_sem, to_tile, to_line, to_core):
        return pltpu.make_async_remote_copy(
            src_ref=src,
            dst_ref=dst,
            send_sem=out_sem,
            recv_sem=in_sem,
            device_id={"tile": to_tile, "kern": to_line, "cond": to_core},
            device_id_type=MESH,
        )

    def arrived(ref, sem):
        pltpu.make_async_copy(ref, ref, sem).wait()

    barrier = pltpu.get_barrier_semaphore()
    for step in range(tile - 1, 0, -1):
        for flip in range(cond):
            pl.semaphore_signal(
                barrier,
                inc=1,
                device_id={
                    "tile": lax.rem(me + step, tile),
                    "kern": line,
                    "cond": lax.rem(core + flip, cond),
                },
                device_id_type=MESH,
            )
    pl.semaphore_signal(
        barrier, inc=1, device_id={"tile": me, "kern": line, "cond": 1 - core}, device_id_type=MESH
    )
    for shift in range(width):
        pl.semaphore_signal(
            barrier,
            inc=1,
            device_id={
                "tile": plane * width + lax.rem(column + shift, width),
                "kern": 1 - line,
                "cond": core,
            },
            device_id_type=MESH,
        )
    greeted = (tile - 1) * cond + 1 + width

    wave_load = pltpu.make_async_copy(wave_hbm, wave, load_sem.at[0])
    kern_load = pltpu.make_async_copy(kern_hbm, held, load_sem.at[1])
    mask_load = pltpu.make_async_copy(mask_hbm, mask_ref, load_sem.at[2])
    weight_load = pltpu.make_async_copy(weight_hbm, weight_ref, load_sem.at[3])
    mask_load.start()
    wave_load.start()
    weight_load.start()
    kern_load.start()

    mask_load.wait()
    wave_load.wait()
    row = jnp.dot(mask_ref[...], wave[...], preferred_element_type=jnp.float32).T
    row_re = row[:count].reshape(tile, cond, part, rows).astype(jnp.bfloat16)
    row_im = (-row[count:]).reshape(tile, cond, part, rows).astype(jnp.bfloat16)
    row_send[:, :, :part, :] = row_re
    row_send[:, :, part:, :] = row_im
    weight[...] = jnp.zeros_like(weight)
    weight_load.wait()
    weight[:conds, :kerns] = weight_ref[...]

    pl.semaphore_wait(barrier, greeted)

    def column_of(origin, side_of):
        return cols.at[side_of, :, pl.ds(pl.multiple_of(origin * rows, rows), rows)]

    def shared(origin):
        return remote(
            column_of(origin, core),
            column_of(origin, core),
            share_out.at[origin],
            share_in.at[origin],
            me,
            line,
            1 - core,
        )

    place = column_of(me, core)
    pltpu.make_async_copy(row_send.at[me, core], place, row_in.at[me]).start()
    for step in range(tile - 1, 0, -1):
        to = lax.rem(me + step, tile)
        remote(
            row_send.at[to, core], place, row_out.at[step], row_in.at[me], to, line, core
        ).start()
    pair_copy = remote(
        weight, pairs, pair_out.at[0], pair_in.at[0], me, line, 1 - core
    )
    pair_copy.start()

    for shift in range(width):
        for layer in range(planes // cond):
            at = pl.multiple_of(
                ((core * (planes // cond) + layer) * width + shift) * rows, rows
            )
            to = (shift * (planes // cond) + layer) * rows
            block = wave[pl.ds(at, rows), :].astype(jnp.float32).T.astype(jnp.bfloat16)
            turn[:count, to : to + rows] = block[:count]
            turn[:count, lanes + to : lanes + to + rows] = block[count:]
            turn[count:, to : to + rows] = -block[count:]
            turn[count:, lanes + to : lanes + to + rows] = block[:count]
    for step in range(steps):
        back[step, :wide, :] = wave[step * wide : (step + 1) * wide, :count]
        back[step, wide:, :] = wave[step * wide : (step + 1) * wide, count:]
    pack = 16
    first = lax.broadcasted_iota(jnp.int32, (pack, count), 0) == 0
    middle = jnp.broadcast_to(
        wave[pixels // 2 : pixels // 2 + pack, :count].astype(jnp.float32)[:1], (pack, count)
    )
    back[0, wide : wide + pack, :] = jnp.where(
        first, middle, wave[:pack, count:].astype(jnp.float32)
    ).astype(jnp.bfloat16)
    power[...] = jnp.zeros_like(power)
    cross[...] = jnp.zeros_like(cross)

    order = (
        plane,
        plane + 1 - 2 * lax.rem(plane, 2),
        lax.rem(plane + planes // 2, planes),
        planes - 1 - plane,
    )
    nearest = [at * width + shift for at in order for shift in range(width)]
    for origin in nearest:
        arrived(column_of(origin, core), row_in.at[origin])
        shared(origin).start()
    for origin in nearest:
        arrived(column_of(origin, 1 - core), share_in.at[origin])
    mixed = jnp.dot(
        cols[...].reshape(2 * freqs, pixels), wave[...], preferred_element_type=jnp.float32
    )
    for other in range(cond):
        re = mixed[2 * other * part : (2 * other + 1) * part]
        im = mixed[(2 * other + 1) * part : (2 * other + 2) * part]
        spec[0, other * part : (other + 1) * part] = re[:, :count] + im[:, count:]
        spec[1, other * part : (other + 1) * part] = im[:, :count] - re[:, count:]
    kern_load.wait()

    blocks = [(layer, shift) for layer in range(conds) for shift in range(width)]

    def targets(layer, shift):
        to = (core * conds + layer) * width + shift
        for other in range(cond):
            index = (layer * width + shift) * cond + other
            yield index, other, to, jnp.logical_and(to == me, other == core)

    def filter_block(item, layer, shift):
        slot = shift * items + item
        for at in range(0, freqs, pack):
            near = pl.ds(at, pack)
            kern_re = held[0, layer, slot, near, :].astype(jnp.float32)
            kern_im = held[1, layer, slot, near, :].astype(jnp.float32)
            spec_re = spec[0, near, :]
            spec_im = spec[1, near, :]
            filt[layer, slot, near, :count] = (spec_re * kern_re - spec_im * kern_im).astype(
                jnp.bfloat16
            )
            filt[layer, slot, near, count:] = (spec_re * kern_im + spec_im * kern_re).astype(
                jnp.bfloat16
            )

    def send_block(item, layer, shift):
        for index, other, to, mine in targets(layer, shift):
            src = filt.at[layer, shift * items + item, pl.ds(other * part, part)]
            dst = recv.at[item, me, pl.ds(other * part, part)]

            @pl.when(mine)
            def _():
                pltpu.make_async_copy(src, dst, send_in.at[item, me]).start()

            @pl.when(jnp.logical_not(mine))
            def _():
                remote(
                    src, dst, send_out.at[item, index], send_in.at[item, me], to, line, other
                ).start()

    def source_step(item, carry):
        for index, block in enumerate(blocks):
            filter_block(item, *block)
            if index:
                send_block(item, *blocks[index - 1])
            else:

                @pl.when(item > 0)
                def _():
                    send_block(item - 1, *blocks[-1])

        return carry

    lax.fori_loop(0, items, source_step, 0)
    send_block(items - 1, *blocks[-1])

    pair_copy.wait()
    weights = jnp.where(source == core, weight[...], pairs[...])
    lane = lax.broadcasted_iota(jnp.int32, weights.shape, 1)
    level = lax.broadcasted_iota(jnp.int32, weights.shape, 0)
    weights = jnp.where(level == lax.rem(plane, conds), weights, 0.0)
    sign = jnp.where(line == 0, 2.0, -2.0)
    mine_half = pl.ds(pl.multiple_of(core * part, part), part)
    their_half = pl.ds(pl.multiple_of((1 - core) * part, part), part)

    def passed(item, origin):
        return remote(
            recv.at[item, origin, mine_half],
            recv.at[item, origin, mine_half],
            pass_out.at[item, origin],
            pass_in.at[item, origin],
            me,
            line,
            1 - core,
        )

    peers = [(1, 1), (1, 0), (0, 1)]

    def quarter(index, piece):
        turn_x, turn_y = peers[index]
        to_column = lax.rem(column + turn_x, width)
        to_line = lax.rem(line + turn_y, kern)
        span = pl.ds(piece * chunk, chunk)
        return remote(
            quarter_send.at[to_line, to_column, span],
            quarter_recv.at[index, span],
            quarter_out.at[piece, index],
            quarter_in.at[piece, index],
            plane * width + to_column,
            to_line,
            core,
        )

    def item_step(item, carry):
        def ready(index):
            for shift in range(width):
                origin = nearest[index * width + shift]
                arrived(recv.at[item, origin, their_half], pass_in.at[item, origin])
            first = order[index] * width
            block = recv[item, pl.ds(first, width)].reshape(width * freqs, 2 * count)
            into = pl.ds(pl.multiple_of(first * freqs, width * freqs), width * freqs)
            half[into, :] = jnp.dot(
                block, turn[...], preferred_element_type=jnp.float32
            ).astype(jnp.bfloat16)

        for index in range(planes):
            for shift in range(width):
                origin = nearest[index * width + shift]
                arrived(recv.at[item, origin, mine_half], send_in.at[item, origin])
                passed(item, origin).start()
            if index:
                ready(index - 1)
        ready(planes - 1)
        scale = jnp.sum(jnp.where(lane == column * items + item, weights, 0.0))

        def pixel_step(step, carry):
            grid[...] = jnp.dot(back[step], half[...], preferred_element_type=jnp.float32)

            def group(at, carry):
                near = pl.ds(pl.multiple_of(at * pack, pack), pack)
                far = pl.ds(pl.multiple_of(wide + at * pack, pack), pack)
                a_re = grid[near, :lanes]
                a_im = grid[near, lanes:]
                b_re = grid[far, :lanes]
                b_im = grid[far, lanes:]
                into = pl.ds(pl.multiple_of(step * wide + at * pack, pack), pack)
                power[into, :] += scale * (
                    (a_re * a_re + a_im * a_im) + (b_re * b_re + b_im * b_im)
                )
                cross[into, :] += scale * (a_im * b_re - a_re * b_im)
                return carry

            lax.fori_loop(0, wide // pack, group, 0)

            @pl.when(step == 0)
            def _():
                top = 8
                a_re = grid[:top, :lanes]
                a_im = grid[:top, lanes:]
                b_re = grid[wide : wide + top, :lanes]
                b_im = grid[wide : wide + top, lanes:]
                a = a_re * a_re + a_im * a_im
                b = b_re * b_re + b_im * b_im
                only = lax.broadcasted_iota(jnp.int32, (top, lanes), 0) == 0
                power[:top, :] -= jnp.where(only, (0.5 * scale) * (a + b), 0.0)
                cross[:top, :] += jnp.where(
                    only, scale * (0.25 * (a - b) - (a_im * b_re - a_re * b_im)), 0.0
                )

            @pl.when(item == items - 1)
            def _():
                for piece in range(wide // chunk):

                    def finish(at, carry):
                        into = pl.ds(
                            pl.multiple_of(step * wide + piece * chunk + at * pack, pack), pack
                        )
                        total = power[into, :]
                        twice = 2.0 * cross[into, :]
                        for shift in range(width):
                            own = slice(shift * side, (shift + 1) * side)
                            quarter_send[0, shift, into, :] = (
                                total[:, own] + twice[:, own]
                            ).astype(jnp.bfloat16)
                            quarter_send[1, shift, into, :] = (
                                total[:, own] - twice[:, own]
                            ).astype(jnp.bfloat16)
                        return carry

                    lax.fori_loop(0, chunk // pack, finish, 0)
                    for index in range(len(peers)):
                        quarter(index, step * (wide // chunk) + piece).start()

            return carry

        lax.fori_loop(0, steps, pixel_step, 0)
        return carry

    lax.fori_loop(0, items, item_step, 0)

    def to_plane(layer, piece, other):
        return remote(
            plane_send.at[layer, pl.ds(piece * chunk, chunk)],
            plane_recv.at[plane, piece],
            plane_out.at[layer, piece, other],
            plane_in.at[plane, piece],
            (core * (planes // cond) + layer) * width + column,
            line,
            other,
        )

    def own_plane(layer, other):
        return jnp.logical_and(core * (planes // cond) + layer == plane, other == core)

    own_side = pl.ds(pl.multiple_of(column * side, side), side)
    for piece in range(pieces):
        for index in range(len(peers)):
            arrived(quarter_recv.at[index, pl.ds(piece * chunk, chunk)], quarter_in.at[piece, index])
        for at in range(piece * chunk, (piece + 1) * chunk, pack):
            span = pl.ds(at, pack)
            total = power[span, own_side] + sign * cross[span, own_side]
            for index in range(len(peers)):
                total = total + quarter_recv[index, span, :].astype(jnp.float32)
            for layer in range(planes // cond):
                plane_send[layer, span, :] = total[:, layer * rows : (layer + 1) * rows].astype(
                    jnp.bfloat16
                )
        for layer in range(planes // cond):
            for other in range(cond):

                @pl.when(own_plane(layer, other))
                def _():
                    pltpu.make_async_copy(
                        plane_send.at[layer, pl.ds(piece * chunk, chunk)],
                        plane_recv.at[plane, piece],
                        plane_in.at[plane, piece],
                    ).start()

                @pl.when(jnp.logical_not(own_plane(layer, other)))
                def _():
                    to_plane(layer, piece, other).start()

    for step in range(1, tile):
        to = lax.rem(me + step, tile)
        arrived(row_send.at[to, core], row_out.at[step])
    for origin in range(tile):
        shared(origin).wait_send()

    def drain(item, carry):
        for layer, shift in blocks:
            for index, other, to, mine in targets(layer, shift):
                src = filt.at[layer, shift * items + item, pl.ds(other * part, part)]

                @pl.when(jnp.logical_not(mine))
                def _():
                    arrived(src, send_out.at[item, index])

        for origin in range(tile):
            arrived(recv.at[item, origin, mine_half], pass_out.at[item, origin])
        return carry

    lax.fori_loop(0, items, drain, 0)
    for piece in range(pieces):
        for index in range(len(peers)):
            quarter(index, piece).wait_send()
        for layer in range(planes // cond):
            for other in range(cond):

                @pl.when(jnp.logical_not(own_plane(layer, other)))
                def _():
                    to_plane(layer, piece, other).wait_send()

    for piece in range(pieces):
        for layer in range(planes):
            arrived(plane_recv.at[layer, piece], plane_in.at[layer, piece])
        for at in range(0, chunk, pack):
            values = [
                plane_recv[layer, piece, at : at + pack, :].astype(jnp.float32)
                for layer in range(planes)
            ]
            into = pl.ds(piece * chunk + at, pack)
            out_ref[0, into, :] = functools.reduce(jnp.minimum, values).astype(jnp.bfloat16)
            out_ref[1, into, :] = functools.reduce(jnp.maximum, values).astype(jnp.bfloat16)


def fused(sizes, mask, kernels, weights, wave):
    tile, kern, cond = sizes
    rows, pixels = mask.shape
    _, conds, kerns, freqs, count = kernels.shape
    planes = conds * cond
    width = tile // planes
    items = kerns // width
    lanes = pixels // 2
    wide = 256
    chunk = 128
    steps = lanes // wide
    pieces = lanes // chunk
    peers = width * kern - 1
    dma = pltpu.SemaphoreType.DMA
    return pl.pallas_call(
        functools.partial(fused_kernel, sizes),
        out_shape=jax.ShapeDtypeStruct((2, lanes, rows), jnp.bfloat16),
        in_specs=[
            pl.BlockSpec(memory_space=pltpu.HBM),
            pl.BlockSpec(memory_space=pltpu.HBM),
            pl.BlockSpec(memory_space=pltpu.HBM),
            pl.BlockSpec(memory_space=pltpu.HBM),
        ],
        out_specs=pl.BlockSpec(memory_space=pltpu.VMEM),
        scratch_shapes=[
            pltpu.VMEM((pixels, 2 * count), jnp.bfloat16),
            pltpu.VMEM(kernels.shape, jnp.bfloat16),
            pltpu.VMEM((tile, cond, 2 * freqs // cond, rows), jnp.bfloat16),
            pltpu.VMEM((cond, 2 * freqs // cond, pixels), jnp.bfloat16),
            pltpu.VMEM((2, freqs, count), jnp.float32),
            pltpu.VMEM((conds, kerns, freqs, 2 * count), jnp.bfloat16),
            pltpu.VMEM((items, tile, freqs, 2 * count), jnp.bfloat16),
            pltpu.VMEM((2 * count, pixels), jnp.bfloat16),
            pltpu.VMEM((steps, 2 * wide, count), jnp.bfloat16),
            pltpu.VMEM((count, pixels), jnp.bfloat16),
            pltpu.VMEM((2 * wide, pixels), jnp.float32),
            pltpu.VMEM((lanes, lanes), jnp.float32),
            pltpu.VMEM((lanes, lanes), jnp.float32),
            pltpu.VMEM((8, 128), jnp.float32),
            pltpu.VMEM((kern, width, lanes, lanes // width), jnp.bfloat16),
            pltpu.VMEM((peers, lanes, lanes // width), jnp.bfloat16),
            pltpu.VMEM((planes // cond, lanes, rows), jnp.bfloat16),
            pltpu.VMEM((planes, pieces, chunk, rows), jnp.bfloat16),
            dma((4,)),
            dma((tile,)),
            dma((tile,)),
            dma((tile,)),
            dma((tile,)),
            dma((1,)),
            dma((1,)),
            dma((items, tile)),
            dma((items, tile)),
            dma((items, tile)),
            dma((items, tile)),
            dma((pieces, peers)),
            dma((pieces, peers)),
            dma((planes // cond, pieces, cond)),
            dma((planes, pieces)),
            pltpu.VMEM((8, 128), jnp.float32),
            pltpu.VMEM(weights.shape, jnp.float32),
            pltpu.VMEM(mask.shape, jnp.bfloat16),
        ],
        compiler_params=pltpu.CompilerParams(
            collective_id=0, has_side_effects=True, vmem_limit_bytes=48 * 1024 * 1024
        ),
    )(mask, weights, wave, kernels)


def place_kernel(final, low_hbm, high_hbm, placed, store_sem):
    line = lax.axis_index("kern")
    size = final.shape[1]
    slot = lax.broadcasted_iota(jnp.int32, (size, size), 0)
    pixel = lax.broadcasted_iota(jnp.int32, (size, size), 1)
    wanted = jnp.where(line == 0, pixel, jnp.where(pixel == 0, 0, size - pixel))
    order = (slot == wanted).astype(jnp.bfloat16)
    stores = []
    for index, target in enumerate((low_hbm, high_hbm)):
        placed[index] = lax.dot_general(
            final[index], order, (((0,), (0,)), ((), ())), preferred_element_type=jnp.float32
        )
        stores.append(pltpu.make_async_copy(placed.at[index], target.at[0], store_sem.at[index]))
        stores[-1].start()
    for store in stores:
        store.wait()


def planes_of(sizes, mask, kernels, kernel_weights):
    _, rows, pixels = mask.shape
    count = kernels.shape[4]
    conds, kerns = kernel_weights.shape
    cos, sin = host_tables(pixels, count)
    wave = jnp.asarray(np.concatenate([cos, sin], axis=1), jnp.bfloat16)
    final = fused(
        sizes,
        *(
            pltpu.with_memory_space_constraint(value, pltpu.HBM)
            for value in (mask[0], kernels, kernel_weights, wave)
        ),
    )
    shape = jax.ShapeDtypeStruct((1, rows, pixels // 2), jnp.float32)
    anywhere = pl.BlockSpec(memory_space=pltpu.HBM)
    return pl.pallas_call(
        place_kernel,
        out_shape=(shape, shape),
        in_specs=[pl.BlockSpec(memory_space=pltpu.VMEM)],
        out_specs=(anywhere, anywhere),
        scratch_shapes=[
            pltpu.VMEM((2, rows, pixels // 2), jnp.float32),
            pltpu.SemaphoreType.DMA((2,)),
        ],
        compiler_params=pltpu.CompilerParams(vmem_limit_bytes=8 * 1024 * 1024),
    )(final)


def plan(mesh):
    tile, kern, cond = (mesh.shape[name] for name in ("tile", "kern", "cond"))

    def body(mask, kernels, kernel_weights):
        conds, kerns = kernel_weights.shape
        freqs, count = kernels.shape[3:]
        rows, pixels = mask.shape[1:]
        split = kern == 2 and cond == 2 and conds == 2 and tile == 2 * conds * cond
        split = split and mask.shape[0] == 1 and count * 2 == pixels and kerns % 2 == 0
        split = split and rows == 128 and freqs % 32 == 0 and pixels == tile * rows
        if split and kerns <= 128 and count % 512 == 0:
            return planes_of((tile, kern, cond), mask, kernels, kernel_weights)
        return local(mask, kernels, kernel_weights)

    return body


def solution(mesh):
    placed = (P(None, "tile", None), P(None, "cond", "kern", "tile", None), P("cond", "kern"))
    return jax.shard_map(
        plan(mesh),
        mesh=mesh,
        in_specs=placed,
        out_specs=(P(None, "tile", "kern"), P(None, "tile", "kern")),
        check_vma=False,
    )
```

```python
import functools
import math

import jax
import jax.numpy as jnp
import numpy as np
from jax import lax
from jax.experimental import pallas as pl
from jax.experimental.pallas import tpu as pltpu
from jax.sharding import PartitionSpec as P


def tables(length, count):
    pixel = jnp.arange(length, dtype=jnp.int32)[:, None]
    freq = jnp.arange(count, dtype=jnp.int32)[None, :] - count // 2
    phase = jnp.mod(pixel * freq, length).astype(jnp.float32) * (2.0 * math.pi / length)
    factor = 1.0 / math.sqrt(length)
    return (
        (jnp.cos(phase) * factor).astype(jnp.bfloat16),
        (jnp.sin(phase) * factor).astype(jnp.bfloat16),
    )


def field_power(half_re, half_im, cos_table, sin_table):
    field_re = jnp.einsum("tnjr,pj->tnrp", half_re, cos_table, preferred_element_type=jnp.float32)
    field_re = field_re - jnp.einsum(
        "tnjr,pj->tnrp", half_im, sin_table, preferred_element_type=jnp.float32
    )
    field_im = jnp.einsum("tnjr,pj->tnrp", half_re, sin_table, preferred_element_type=jnp.float32)
    field_im = field_im + jnp.einsum(
        "tnjr,pj->tnrp", half_im, cos_table, preferred_element_type=jnp.float32
    )
    return field_re * field_re + field_im * field_im


def filter_spectrum(spec_re, spec_im, kern_re, kern_im):
    kern_re = kern_re.astype(jnp.float32)
    kern_im = kern_im.astype(jnp.float32)
    filt_re = spec_re[:, None] * kern_re[None] - spec_im[:, None] * kern_im[None]
    filt_im = spec_re[:, None] * kern_im[None] + spec_im[:, None] * kern_re[None]
    return (filt_re.astype(jnp.bfloat16), filt_im.astype(jnp.bfloat16))


def half_transform(filt_re, filt_im, cos_part, sin_part):
    half_re = jnp.einsum("tnji,ri->tnjr", filt_re, cos_part, preferred_element_type=jnp.float32)
    half_re = half_re - jnp.einsum(
        "tnji,ri->tnjr", filt_im, sin_part, preferred_element_type=jnp.float32
    )
    half_im = jnp.einsum("tnji,ri->tnjr", filt_re, sin_part, preferred_element_type=jnp.float32)
    half_im = half_im + jnp.einsum(
        "tnji,ri->tnjr", filt_im, cos_part, preferred_element_type=jnp.float32
    )
    return (half_re.astype(jnp.bfloat16), half_im.astype(jnp.bfloat16))


def column_spectrum(rows_re, rows_im, cos_part, sin_part):
    spec_re = jnp.einsum("tjr,ri->tji", rows_re, cos_part, preferred_element_type=jnp.float32)
    spec_re = spec_re + jnp.einsum(
        "tjr,ri->tji", rows_im, sin_part, preferred_element_type=jnp.float32
    )
    spec_im = jnp.einsum("tjr,ri->tji", rows_im, cos_part, preferred_element_type=jnp.float32)
    spec_im = spec_im - jnp.einsum(
        "tjr,ri->tji", rows_re, sin_part, preferred_element_type=jnp.float32
    )
    return (spec_re, spec_im)


def local(mask, kernels, kernel_weights):
    tiles_here, rows, pixels = mask.shape
    count = kernels.shape[4]
    conds, kerns = kernel_weights.shape
    items = conds * kerns
    cos_table, sin_table = tables(pixels, count)
    row_re = jnp.einsum("trc,cj->tjr", mask, cos_table, preferred_element_type=jnp.float32).astype(
        jnp.bfloat16
    )
    row_im = (
        -jnp.einsum("trc,cj->tjr", mask, sin_table, preferred_element_type=jnp.float32)
    ).astype(jnp.bfloat16)
    cols_re, cols_im = (
        lax.all_to_all(row_re, "tile", split_axis=1, concat_axis=2, tiled=True),
        lax.all_to_all(row_im, "tile", split_axis=1, concat_axis=2, tiled=True),
    )
    spec_re, spec_im = column_spectrum(cols_re, cols_im, cos_table, sin_table)
    freq_here = kernels.shape[3]
    kern_re = kernels[0].reshape(items, freq_here, count)
    kern_im = kernels[1].reshape(items, freq_here, count)
    filt_re, filt_im = filter_spectrum(spec_re, spec_im, kern_re, kern_im)
    half_re, half_im = half_transform(filt_re, filt_im, cos_table, sin_table)
    power = field_power(
        lax.all_to_all(half_re, "tile", split_axis=3, concat_axis=2, tiled=True),
        lax.all_to_all(half_im, "tile", split_axis=3, concat_axis=2, tiled=True),
        cos_table,
        sin_table,
    )
    power = power.reshape(tiles_here, conds, kerns, rows, pixels)
    weighted = jnp.einsum("tckrp,ck->tcrp", power, kernel_weights, precision=lax.Precision.HIGHEST)
    intensity = lax.psum_scatter(weighted, "kern", scatter_dimension=3, tiled=True)
    local_low = jnp.min(intensity, axis=1)
    local_high = jnp.max(intensity, axis=1)
    low = lax.pmin(local_low, "cond")
    high = lax.pmax(local_high, "cond")
    return (low, high)


def host_tables(length, count):
    pixel = np.arange(length, dtype=np.int64)[:, None]
    freq = np.arange(count, dtype=np.int64)[None, :] - count // 2
    phase = np.mod(pixel * freq, length).astype(np.float64) * (2.0 * math.pi / length)
    factor = 1.0 / math.sqrt(length)
    return np.cos(phase) * factor, np.sin(phase) * factor


MESH = pl.DeviceIdType.MESH


def fused_kernel(sizes, mask_hbm, weight_hbm, wave_hbm, kern_hbm, out_ref, *scratch):
    tile, kern, cond = sizes
    (wave, held, row_send, cols, spec, filt, recv, turn, back, half, grid, power, cross, pairs) = scratch[:14]
    (quarter_send, first_recv, second_send, second_recv, keep) = scratch[14:19]
    (plane_send, plane_recv, final) = scratch[19:22]
    weight, weight_ref, mask_ref = scratch[-3:]
    (load_sem, row_out, row_in, share_out, share_in, pair_out, pair_in) = scratch[22:29]
    (send_out, send_in, pass_out, pass_in) = scratch[29:33]
    (first_out, first_in, second_out, second_in) = scratch[33:37]
    (plane_out, plane_in, final_out, final_in) = scratch[37:41]
    rows, pixels = mask_hbm.shape
    _, conds, kerns, freqs, count = kern_hbm.shape
    planes = conds * cond
    width = tile // planes
    items = kerns // width
    part = freqs // cond
    wide = back.shape[1] // 2
    lanes = pixels // 2
    side = lanes // width
    steps = back.shape[0]
    chunk = plane_recv.shape[2]
    pieces = plane_recv.shape[1]
    me = lax.axis_index("tile")
    line = lax.axis_index("kern")
    core = lax.axis_index("cond")
    plane = lax.div(me, width)
    column = lax.rem(me, width)
    source = lax.div(plane, conds)

    def remote(src, dst, out_sem, in_sem, to_tile, to_line, to_core):
        return pltpu.make_async_remote_copy(
            src_ref=src,
            dst_ref=dst,
            send_sem=out_sem,
            recv_sem=in_sem,
            device_id={"tile": to_tile, "kern": to_line, "cond": to_core},
            device_id_type=MESH,
        )

    def arrived(ref, sem):
        pltpu.make_async_copy(ref, ref, sem).wait()

    barrier = pltpu.get_barrier_semaphore()
    for step in range(tile - 1, 0, -1):
        for flip in range(cond):
            pl.semaphore_signal(
                barrier,
                inc=1,
                device_id={
                    "tile": lax.rem(me + step, tile),
                    "kern": line,
                    "cond": lax.rem(core + flip, cond),
                },
                device_id_type=MESH,
            )
    pl.semaphore_signal(
        barrier, inc=1, device_id={"tile": me, "kern": line, "cond": 1 - core}, device_id_type=MESH
    )
    for shift in range(width):
        pl.semaphore_signal(
            barrier,
            inc=1,
            device_id={
                "tile": plane * width + lax.rem(column + shift, width),
                "kern": 1 - line,
                "cond": core,
            },
            device_id_type=MESH,
        )
    greeted = (tile - 1) * cond + 1 + width

    wave_load = pltpu.make_async_copy(wave_hbm, wave, load_sem.at[0])
    kern_load = pltpu.make_async_copy(kern_hbm, held, load_sem.at[1])
    mask_load = pltpu.make_async_copy(mask_hbm, mask_ref, load_sem.at[2])
    weight_load = pltpu.make_async_copy(weight_hbm, weight_ref, load_sem.at[3])
    mask_load.start()
    wave_load.start()
    weight_load.start()
    kern_load.start()

    mask_load.wait()
    wave_load.wait()
    row = jnp.dot(mask_ref[...], wave[...], preferred_element_type=jnp.float32).T
    row_re = row[:count].reshape(tile, cond, part, rows).astype(jnp.bfloat16)
    row_im = (-row[count:]).reshape(tile, cond, part, rows).astype(jnp.bfloat16)
    row_send[:, :, :part, :] = row_re
    row_send[:, :, part:, :] = row_im
    weight[...] = jnp.zeros_like(weight)
    weight_load.wait()
    weight[:conds, :kerns] = weight_ref[...]

    pl.semaphore_wait(barrier, greeted)

    def column_of(origin, side_of):
        return cols.at[side_of, :, pl.ds(pl.multiple_of(origin * rows, rows), rows)]

    def shared(origin):
        return remote(
            column_of(origin, core),
            column_of(origin, core),
            share_out.at[origin],
            share_in.at[origin],
            me,
            line,
            1 - core,
        )

    place = column_of(me, core)
    pltpu.make_async_copy(row_send.at[me, core], place, row_in.at[me]).start()
    for step in range(tile - 1, 0, -1):
        to = lax.rem(me + step, tile)
        remote(
            row_send.at[to, core], place, row_out.at[step], row_in.at[me], to, line, core
        ).start()
    pair_copy = remote(
        weight, pairs, pair_out.at[0], pair_in.at[0], me, line, 1 - core
    )
    pair_copy.start()

    pack = 16

    order = (
        plane,
        plane + 1 - 2 * lax.rem(plane, 2),
        lax.rem(plane + planes // 2, planes),
        planes - 1 - plane,
    )
    nearest = [at * width + shift for at in order for shift in range(width)]
    for origin in nearest:
        arrived(column_of(origin, core), row_in.at[origin])
        shared(origin).start()
    for origin in nearest:
        arrived(column_of(origin, 1 - core), share_in.at[origin])
    mixed = jnp.dot(
        cols[...].reshape(2 * freqs, pixels), wave[...], preferred_element_type=jnp.float32
    )
    for other in range(cond):
        re = mixed[2 * other * part : (2 * other + 1) * part]
        im = mixed[(2 * other + 1) * part : (2 * other + 2) * part]
        spec[0, other * part : (other + 1) * part] = re[:, :count] + im[:, count:]
        spec[1, other * part : (other + 1) * part] = im[:, :count] - re[:, count:]
    kern_load.wait()

    blocks = [(layer, shift) for layer in range(conds) for shift in range(width)]

    def targets(layer, shift):
        to = (core * conds + layer) * width + shift
        for other in range(cond):
            index = (layer * width + shift) * cond + other
            yield index, other, to, jnp.logical_and(to == me, other == core)

    def filter_block(item, layer, shift):
        slot = shift * items + item
        for at in range(0, freqs, pack):
            near = pl.ds(at, pack)
            kern_re = held[0, layer, slot, near, :].astype(jnp.float32)
            kern_im = held[1, layer, slot, near, :].astype(jnp.float32)
            spec_re = spec[0, near, :]
            spec_im = spec[1, near, :]
            filt[layer, slot, near, :count] = (spec_re * kern_re - spec_im * kern_im).astype(
                jnp.bfloat16
            )
            filt[layer, slot, near, count:] = (spec_re * kern_im + spec_im * kern_re).astype(
                jnp.bfloat16
            )

    def send_block(item, layer, shift):
        for index, other, to, mine in targets(layer, shift):
            src = filt.at[layer, shift * items + item, pl.ds(other * part, part)]
            dst = recv.at[item, me, pl.ds(other * part, part)]

            @pl.when(mine)
            def _():
                pltpu.make_async_copy(src, dst, send_in.at[item, me]).start()

            @pl.when(jnp.logical_not(mine))
            def _():
                remote(
                    src, dst, send_out.at[item, index], send_in.at[item, me], to, line, other
                ).start()

    def source_step(item, carry):
        for index, block in enumerate(blocks):
            filter_block(item, *block)
            if index:
                send_block(item, *blocks[index - 1])
            else:

                @pl.when(item > 0)
                def _():
                    send_block(item - 1, *blocks[-1])

        return carry

    lax.fori_loop(0, items, source_step, 0)
    send_block(items - 1, *blocks[-1])

    for shift in range(width):
        for layer in range(planes // cond):
            at = pl.multiple_of(
                ((core * (planes // cond) + layer) * width + shift) * rows, rows
            )
            to = (shift * (planes // cond) + layer) * rows
            block = wave[pl.ds(at, rows), :].astype(jnp.float32).T.astype(jnp.bfloat16)
            turn[:count, to : to + rows] = block[:count]
            turn[:count, lanes + to : lanes + to + rows] = block[count:]
            turn[count:, to : to + rows] = -block[count:]
            turn[count:, lanes + to : lanes + to + rows] = block[:count]
    for step in range(steps):
        back[step, :wide, :] = wave[step * wide : (step + 1) * wide, :count]
        back[step, wide:, :] = wave[step * wide : (step + 1) * wide, count:]
    first = lax.broadcasted_iota(jnp.int32, (pack, count), 0) == 0
    middle = jnp.broadcast_to(
        wave[pixels // 2 : pixels // 2 + pack, :count].astype(jnp.float32)[:1], (pack, count)
    )
    back[0, wide : wide + pack, :] = jnp.where(
        first, middle, wave[:pack, count:].astype(jnp.float32)
    ).astype(jnp.bfloat16)
    power[...] = jnp.zeros_like(power)
    cross[...] = jnp.zeros_like(cross)

    pair_copy.wait()
    weights = jnp.where(source == core, weight[...], pairs[...])
    lane = lax.broadcasted_iota(jnp.int32, weights.shape, 1)
    level = lax.broadcasted_iota(jnp.int32, weights.shape, 0)
    weights = jnp.where(level == lax.rem(plane, conds), weights, 0.0)
    sign = jnp.where(line == 0, 2.0, -2.0)
    mine_half = pl.ds(pl.multiple_of(core * part, part), part)
    their_half = pl.ds(pl.multiple_of((1 - core) * part, part), part)

    def passed(item, origin):
        return remote(
            recv.at[item, origin, mine_half],
            recv.at[item, origin, mine_half],
            pass_out.at[item, origin],
            pass_in.at[item, origin],
            me,
            line,
            1 - core,
        )

    def first(piece):
        span = pl.ds(piece * chunk, chunk)
        along_x = piece % 2 == 0
        return remote(
            quarter_send.at[:, 1 - column, span] if along_x else quarter_send.at[1 - line, :, span],
            first_recv.at[:, span],
            first_out.at[piece],
            first_in.at[piece],
            plane * width + (1 - column) if along_x else me,
            line if along_x else 1 - line,
            core,
        )

    def second(piece):
        span = pl.ds(piece * chunk, chunk)
        along_x = piece % 2 == 1
        return remote(
            second_send.at[span],
            second_recv.at[span],
            second_out.at[piece],
            second_in.at[piece],
            plane * width + (1 - column) if along_x else me,
            line if along_x else 1 - line,
            core,
        )

    ahead = 4
    lag = 3

    def item_step(item, carry):
        def ready(index):
            for shift in range(width):
                origin = nearest[index * width + shift]
                arrived(recv.at[item, origin, their_half], pass_in.at[item, origin])
            first = order[index] * width
            block = recv[item, pl.ds(first, width)].reshape(width * freqs, 2 * count)
            into = pl.ds(pl.multiple_of(first * freqs, width * freqs), width * freqs)
            half[into, :] = jnp.dot(
                block, turn[...], preferred_element_type=jnp.float32
            ).astype(jnp.bfloat16)

        for index in range(planes):
            for shift in range(width):
                origin = nearest[index * width + shift]
                arrived(recv.at[item, origin, mine_half], send_in.at[item, origin])
                passed(item, origin).start()
            if index:
                ready(index - 1)
        ready(planes - 1)
        scale = jnp.sum(jnp.where(lane == column * items + item, weights, 0.0))

        def pixel_step(step, carry):
            grid[...] = jnp.dot(back[step], half[...], preferred_element_type=jnp.float32)

            def group(at, carry):
                near = pl.ds(pl.multiple_of(at * pack, pack), pack)
                far = pl.ds(pl.multiple_of(wide + at * pack, pack), pack)
                a_re = grid[near, :lanes]
                a_im = grid[near, lanes:]
                b_re = grid[far, :lanes]
                b_im = grid[far, lanes:]
                into = pl.ds(pl.multiple_of(step * wide + at * pack, pack), pack)
                power[into, :] += scale * (
                    (a_re * a_re + a_im * a_im) + (b_re * b_re + b_im * b_im)
                )
                cross[into, :] += scale * (a_im * b_re - a_re * b_im)
                return carry

            lax.fori_loop(0, wide // pack, group, 0)

            @pl.when(step == 0)
            def _():
                top = 8
                a_re = grid[:top, :lanes]
                a_im = grid[:top, lanes:]
                b_re = grid[wide : wide + top, :lanes]
                b_im = grid[wide : wide + top, lanes:]
                a = a_re * a_re + a_im * a_im
                b = b_re * b_re + b_im * b_im
                only = lax.broadcasted_iota(jnp.int32, (top, lanes), 0) == 0
                power[:top, :] -= jnp.where(only, (0.5 * scale) * (a + b), 0.0)
                cross[:top, :] += jnp.where(
                    only, scale * (0.25 * (a - b) - (a_im * b_re - a_re * b_im)), 0.0
                )

            @pl.when(item == items - 1)
            def _():
                for piece in range(wide // chunk):

                    def finish(at, carry):
                        into = pl.ds(
                            pl.multiple_of(step * wide + piece * chunk + at * pack, pack), pack
                        )
                        total = power[into, :]
                        twice = 2.0 * cross[into, :]
                        for shift in range(width):
                            own = slice(shift * side, (shift + 1) * side)
                            quarter_send[0, shift, into, :] = (
                                total[:, own] + twice[:, own]
                            ).astype(jnp.bfloat16)
                            quarter_send[1, shift, into, :] = (
                                total[:, own] - twice[:, own]
                            ).astype(jnp.bfloat16)
                        return carry

                    lax.fori_loop(0, chunk // pack, finish, 0)

                    for begun in range(steps):

                        @pl.when(step == begun)
                        def _():
                            if begun * (wide // chunk) + piece < ahead:
                                first(begun * (wide // chunk) + piece).start()

            return carry

        lax.fori_loop(0, steps, pixel_step, 0)
        return carry

    lax.fori_loop(0, items, item_step, 0)

    both = pieces - 0

    def owners(piece):
        return range(cond) if piece >= both else (piece % cond,)

    def to_plane(layer, piece, other):
        return remote(
            plane_send.at[layer, pl.ds(piece * chunk, chunk)],
            plane_recv.at[plane, piece],
            plane_out.at[layer, piece, other],
            plane_in.at[plane, piece],
            (core * (planes // cond) + layer) * width + column,
            line,
            other,
        )

    def own_plane(layer, other):
        return jnp.logical_and(core * (planes // cond) + layer == plane, other == core)

    own_side = pl.ds(pl.multiple_of(column * side, side), side)
    their_side = pl.ds(pl.multiple_of((1 - column) * side, side), side)

    def combine(piece):
        arrived(first_recv.at[:, pl.ds(piece * chunk, chunk)], first_in.at[piece])
        for at in range(piece * chunk, (piece + 1) * chunk, pack):
            span = pl.ds(at, pack)
            kept = power[span, own_side] + sign * cross[span, own_side]
            if piece % 2 == 0:
                given = power[span, own_side] - sign * cross[span, own_side]
                index = line
            else:
                given = power[span, their_side] + sign * cross[span, their_side]
                index = column
            keep[span, :] = kept + first_recv[index, span, :].astype(jnp.float32)
            second_send[span, :] = (
                given + first_recv[1 - index, span, :].astype(jnp.float32)
            ).astype(jnp.bfloat16)
        second(piece).start()

    def complete(piece):
        arrived(second_recv.at[pl.ds(piece * chunk, chunk)], second_in.at[piece])
        for at in range(piece * chunk, (piece + 1) * chunk, pack):
            span = pl.ds(at, pack)
            total = keep[span, :] + second_recv[span, :].astype(jnp.float32)
            for layer in range(planes // cond):
                plane_send[layer, span, :] = total[:, layer * rows : (layer + 1) * rows].astype(
                    jnp.bfloat16
                )
        for layer in range(planes // cond):
            for other in owners(piece):

                @pl.when(own_plane(layer, other))
                def _():
                    pltpu.make_async_copy(
                        plane_send.at[layer, pl.ds(piece * chunk, chunk)],
                        plane_recv.at[plane, piece],
                        plane_in.at[plane, piece],
                    ).start()

                @pl.when(jnp.logical_not(own_plane(layer, other)))
                def _():
                    to_plane(layer, piece, other).start()

    for piece in range(pieces + lag):
        if piece < pieces:
            combine(piece)
            if piece + ahead < pieces:
                first(piece + ahead).start()
        if piece >= lag:
            complete(piece - lag)

    def reduce(piece):
        for layer in range(planes):
            arrived(plane_recv.at[layer, piece], plane_in.at[layer, piece])
        for at in range(0, chunk, pack):
            values = [
                plane_recv[layer, piece, at : at + pack, :].astype(jnp.float32)
                for layer in range(planes)
            ]
            into = pl.ds(pl.multiple_of(piece * chunk + at, pack), pack)
            final[0, into, :] = functools.reduce(jnp.minimum, values).astype(jnp.bfloat16)
            final[1, into, :] = functools.reduce(jnp.maximum, values).astype(jnp.bfloat16)

    def swap(pair):
        span = pl.ds(pl.multiple_of((pair * cond + core) * chunk, chunk), chunk)
        return remote(
            final.at[:, span],
            final.at[:, span],
            final_out.at[pair],
            final_in.at[pair],
            me,
            line,
            1 - core,
        )

    for pair in range(both // cond):
        reduce(pair * cond + core)
        swap(pair).start()
    for piece in range(both, pieces):
        reduce(piece)

    for step in range(1, tile):
        to = lax.rem(me + step, tile)
        arrived(row_send.at[to, core], row_out.at[step])
    for origin in range(tile):
        shared(origin).wait_send()

    def drain(item, carry):
        for layer, shift in blocks:
            for index, other, to, mine in targets(layer, shift):
                src = filt.at[layer, shift * items + item, pl.ds(other * part, part)]

                @pl.when(jnp.logical_not(mine))
                def _():
                    arrived(src, send_out.at[item, index])

        for origin in range(tile):
            arrived(recv.at[item, origin, mine_half], pass_out.at[item, origin])
        return carry

    lax.fori_loop(0, items, drain, 0)
    for piece in range(pieces):
        first(piece).wait_send()
        second(piece).wait_send()
        for layer in range(planes // cond):
            for other in owners(piece):

                @pl.when(jnp.logical_not(own_plane(layer, other)))
                def _():
                    to_plane(layer, piece, other).wait_send()

    for pair in range(both // cond):
        theirs = pl.ds(pl.multiple_of((pair * cond + 1 - core) * chunk, chunk), chunk)
        arrived(final.at[:, theirs], final_in.at[pair])
        swap(pair).wait_send()
    out_ref[...] = final[...]


def fused(sizes, mask, kernels, weights, wave):
    tile, kern, cond = sizes
    rows, pixels = mask.shape
    _, conds, kerns, freqs, count = kernels.shape
    planes = conds * cond
    width = tile // planes
    items = kerns // width
    lanes = pixels // 2
    wide = 256
    chunk = 128
    steps = lanes // wide
    pieces = lanes // chunk
    dma = pltpu.SemaphoreType.DMA
    return pl.pallas_call(
        functools.partial(fused_kernel, sizes),
        out_shape=jax.ShapeDtypeStruct((2, lanes, rows), jnp.bfloat16),
        in_specs=[
            pl.BlockSpec(memory_space=pltpu.HBM),
            pl.BlockSpec(memory_space=pltpu.HBM),
            pl.BlockSpec(memory_space=pltpu.HBM),
            pl.BlockSpec(memory_space=pltpu.HBM),
        ],
        out_specs=pl.BlockSpec(memory_space=pltpu.VMEM),
        scratch_shapes=[
            pltpu.VMEM((pixels, 2 * count), jnp.bfloat16),
            pltpu.VMEM(kernels.shape, jnp.bfloat16),
            pltpu.VMEM((tile, cond, 2 * freqs // cond, rows), jnp.bfloat16),
            pltpu.VMEM((cond, 2 * freqs // cond, pixels), jnp.bfloat16),
            pltpu.VMEM((2, freqs, count), jnp.float32),
            pltpu.VMEM((conds, kerns, freqs, 2 * count), jnp.bfloat16),
            pltpu.VMEM((items, tile, freqs, 2 * count), jnp.bfloat16),
            pltpu.VMEM((2 * count, pixels), jnp.bfloat16),
            pltpu.VMEM((steps, 2 * wide, count), jnp.bfloat16),
            pltpu.VMEM((count, pixels), jnp.bfloat16),
            pltpu.VMEM((2 * wide, pixels), jnp.float32),
            pltpu.VMEM((lanes, lanes), jnp.float32),
            pltpu.VMEM((lanes, lanes), jnp.float32),
            pltpu.VMEM((8, 128), jnp.float32),
            pltpu.VMEM((kern, width, lanes, lanes // width), jnp.bfloat16),
            pltpu.VMEM((2, lanes, lanes // width), jnp.bfloat16),
            pltpu.VMEM((lanes, lanes // width), jnp.bfloat16),
            pltpu.VMEM((lanes, lanes // width), jnp.bfloat16),
            pltpu.VMEM((lanes, lanes // width), jnp.float32),
            pltpu.VMEM((planes // cond, lanes, rows), jnp.bfloat16),
            pltpu.VMEM((planes, pieces, chunk, rows), jnp.bfloat16),
            pltpu.VMEM((2, lanes, rows), jnp.bfloat16),
            dma((4,)),
            dma((tile,)),
            dma((tile,)),
            dma((tile,)),
            dma((tile,)),
            dma((1,)),
            dma((1,)),
            dma((items, tile)),
            dma((items, tile)),
            dma((items, tile)),
            dma((items, tile)),
            dma((pieces,)),
            dma((pieces,)),
            dma((pieces,)),
            dma((pieces,)),
            dma((planes // cond, pieces, cond)),
            dma((planes, pieces)),
            dma((pieces // cond,)),
            dma((pieces // cond,)),
            pltpu.VMEM((8, 128), jnp.float32),
            pltpu.VMEM(weights.shape, jnp.float32),
            pltpu.VMEM(mask.shape, jnp.bfloat16),
        ],
        compiler_params=pltpu.CompilerParams(
            collective_id=0, has_side_effects=True, vmem_limit_bytes=48 * 1024 * 1024
        ),
    )(mask, weights, wave, kernels)


def place_kernel(final, low_hbm, high_hbm, placed, store_sem):
    line = lax.axis_index("kern")
    size = final.shape[1]
    slot = lax.broadcasted_iota(jnp.int32, (size, size), 0)
    pixel = lax.broadcasted_iota(jnp.int32, (size, size), 1)
    wanted = jnp.where(line == 0, pixel, jnp.where(pixel == 0, 0, size - pixel))
    order = (slot == wanted).astype(jnp.bfloat16)
    stores = []
    for index, target in enumerate((low_hbm, high_hbm)):
        placed[index] = lax.dot_general(
            final[index], order, (((0,), (0,)), ((), ())), preferred_element_type=jnp.float32
        )
        stores.append(pltpu.make_async_copy(placed.at[index], target.at[0], store_sem.at[index]))
        stores[-1].start()
    for store in stores:
        store.wait()


def planes_of(sizes, mask, kernels, kernel_weights):
    _, rows, pixels = mask.shape
    count = kernels.shape[4]
    conds, kerns = kernel_weights.shape
    cos, sin = host_tables(pixels, count)
    wave = jnp.asarray(np.concatenate([cos, sin], axis=1), jnp.bfloat16)
    final = fused(
        sizes,
        *(
            pltpu.with_memory_space_constraint(value, pltpu.HBM)
            for value in (mask[0], kernels, kernel_weights, wave)
        ),
    )
    shape = jax.ShapeDtypeStruct((1, rows, pixels // 2), jnp.float32)
    anywhere = pl.BlockSpec(memory_space=pltpu.HBM)
    return pl.pallas_call(
        place_kernel,
        out_shape=(shape, shape),
        in_specs=[pl.BlockSpec(memory_space=pltpu.VMEM)],
        out_specs=(anywhere, anywhere),
        scratch_shapes=[
            pltpu.VMEM((2, rows, pixels // 2), jnp.float32),
            pltpu.SemaphoreType.DMA((2,)),
        ],
        compiler_params=pltpu.CompilerParams(vmem_limit_bytes=8 * 1024 * 1024),
    )(final)


def plan(mesh):
    tile, kern, cond = (mesh.shape[name] for name in ("tile", "kern", "cond"))

    def body(mask, kernels, kernel_weights):
        conds, kerns = kernel_weights.shape
        freqs, count = kernels.shape[3:]
        rows, pixels = mask.shape[1:]
        split = kern == 2 and cond == 2 and conds == 2 and tile == 2 * conds * cond
        split = split and mask.shape[0] == 1 and count * 2 == pixels and kerns % 2 == 0
        split = split and rows == 128 and freqs % 32 == 0 and pixels == tile * rows
        if split and kerns <= 128 and count % 512 == 0:
            return planes_of((tile, kern, cond), mask, kernels, kernel_weights)
        return local(mask, kernels, kernel_weights)

    return body


def solution(mesh):
    placed = (P(None, "tile", None), P(None, "cond", "kern", "tile", None), P("cond", "kern"))
    return jax.shard_map(
        plan(mesh),
        mesh=mesh,
        in_specs=placed,
        out_specs=(P(None, "tile", "kern"), P(None, "tile", "kern")),
        check_vma=False,
    )
```
